128 devices in a mesh: dp: 1, tp: 2 (over core), cp: 64 (over z, y, x).
Axes of the slice: x: 4, y: 4, z: 4, core: 2. Of those that a mesh axis runs over, the one named last changes fastest.
Arguments:
- hidden: bfloat16 [2048, 3072], P(('dp', 'cp'))
- positions: int32 [2048], P(('dp', 'cp'))
- ln_gain: bfloat16 [3072], replicated
- w_q: bfloat16 [3072, 3072], P(None, 'tp')
- w_k: bfloat16 [3072, 1024], P(None, 'tp')
- w_v: bfloat16 [3072, 1024], P(None, 'tp')
- w_o: bfloat16 [3072, 3072], P('tp')
- w_gate: bfloat16 [3072, 8192], P(None, 'tp')
- w_up: bfloat16 [3072, 8192], P(None, 'tp')
- w_down: bfloat16 [8192, 3072], P('tp')
Outputs:
- output 1: bfloat16 [2048, 3072], P(('dp', 'cp'))
- output 2: bfloat16 [2048, 8, 128], P(('dp', 'cp'), 'tp')
- output 3: bfloat16 [2048, 8, 128], P(('dp', 'cp'), 'tp')
All inputs are finite; a program needn't handle non-finite values.
Results may differ from the reference program's by a relative error of at most 0.014011.
Values are sent between devices in bfloat16 or wider.
A program may use at most 1 GiB of HBM per device.

```python
import jax
import jax.numpy as jnp
from jax import lax

D_MODEL = 3072
HEADS = 24
KV_HEADS = 8
FF_DIM = 8192
HEAD_DIM = 128
ROPE_BASE = 4000000
TOKENS = 2048
LN_EPS = 1e-5
Q_BLOCK = min(64, TOKENS)


def layer_norm(hidden, ln_gain):
    hidden_f = hidden.astype(jnp.float32)
    row_mean = jnp.mean(hidden_f, axis=-1, keepdims=True)
    centered = hidden_f - row_mean
    row_var = jnp.mean(centered * centered, axis=-1, keepdims=True)
    return (centered * lax.rsqrt(row_var + LN_EPS) * ln_gain.astype(jnp.float32)).astype(jnp.bfloat16)


def rotary(proj, positions):
    half_dim = HEAD_DIM // 2
    inv_freq = 1.0 / (ROPE_BASE ** (jnp.arange(0, HEAD_DIM, 2, dtype=jnp.float32) / HEAD_DIM))
    angles = positions.astype(jnp.float32)[:, None] * inv_freq[None, :]
    bcast_shape = (proj.shape[0],) + (1,) * (proj.ndim - 2) + (half_dim,)
    cosine = jnp.cos(angles).reshape(bcast_shape)
    sine_val = jnp.sin(angles).reshape(bcast_shape)
    paired = proj.astype(jnp.float32).reshape(proj.shape[:-1] + (half_dim, 2))
    even_part = paired[..., 0]
    odd_part = paired[..., 1]
    rotated = jnp.stack([even_part * cosine - odd_part * sine_val, odd_part * cosine + even_part * sine_val], axis=-1)
    return rotated.reshape(proj.shape).astype(jnp.bfloat16)


def setup_inputs(seed: int = 0, part: int = 0) -> dict:
    base_key = jax.random.key(seed)
    part_keys = jax.random.split(jax.random.fold_in(base_key, part), 2)
    weight_keys = jax.random.split(base_key, 8)
    q_width = HEADS * HEAD_DIM
    kv_width = KV_HEADS * HEAD_DIM
    d_scale = D_MODEL ** -0.5
    hidden = jax.random.normal(part_keys[0], (TOKENS, D_MODEL), jnp.float32)
    pos_steps = jax.random.randint(part_keys[1], (TOKENS,), 1, 3, dtype=jnp.int32)
    positions = (jnp.cumsum(pos_steps, dtype=jnp.int32) - pos_steps[0]).astype(jnp.int32)
    ln_gain = 1.0 + 0.3 * jax.random.normal(weight_keys[0], (D_MODEL,), jnp.float32)
    w_q = (1.5 * d_scale) * jax.random.normal(weight_keys[1], (D_MODEL, q_width), jnp.float32)
    w_k = (1.5 * d_scale) * jax.random.normal(weight_keys[2], (D_MODEL, kv_width), jnp.float32)
    w_v = d_scale * jax.random.normal(weight_keys[3], (D_MODEL, kv_width), jnp.float32)
    w_o = (2.0 * q_width ** -0.5) * jax.random.normal(weight_keys[4], (q_width, D_MODEL), jnp.float32)
    w_gate = d_scale * jax.random.normal(weight_keys[5], (D_MODEL, FF_DIM), jnp.float32)
    w_up = d_scale * jax.random.normal(weight_keys[6], (D_MODEL, FF_DIM), jnp.float32)
    w_down = (FF_DIM ** -0.5) * jax.random.normal(weight_keys[7], (FF_DIM, D_MODEL), jnp.float32)
    return {
        'hidden': hidden.astype(jnp.bfloat16),
        'positions': positions,
        'ln_gain': ln_gain.astype(jnp.bfloat16),
        'w_q': w_q.astype(jnp.bfloat16),
        'w_k': w_k.astype(jnp.bfloat16),
        'w_v': w_v.astype(jnp.bfloat16),
        'w_o': w_o.astype(jnp.bfloat16),
        'w_gate': w_gate.astype(jnp.bfloat16),
        'w_up': w_up.astype(jnp.bfloat16),
        'w_down': w_down.astype(jnp.bfloat16),
    }


def reference(hidden, positions, ln_gain, w_q, w_k, w_v, w_o, w_gate, w_up, w_down):
    group_size = HEADS // KV_HEADS
    normed = layer_norm(hidden, ln_gain)
    q_proj = jnp.dot(normed, w_q, preferred_element_type=jnp.float32).astype(jnp.bfloat16)
    k_proj = jnp.dot(normed, w_k, preferred_element_type=jnp.float32).astype(jnp.bfloat16)
    v_cache = jnp.dot(normed, w_v, preferred_element_type=jnp.float32).astype(jnp.bfloat16).reshape(TOKENS, KV_HEADS, HEAD_DIM)
    q_rot = rotary(q_proj.reshape(TOKENS, KV_HEADS, group_size, HEAD_DIM), positions)
    k_cache = rotary(k_proj.reshape(TOKENS, KV_HEADS, HEAD_DIM), positions)
    k_float = k_cache.astype(jnp.float32)
    v_float = v_cache.astype(jnp.float32)
    key_pos = jnp.arange(TOKENS)
    score_scale = HEAD_DIM ** -0.5
    q_blocks = q_rot.reshape(TOKENS // Q_BLOCK, Q_BLOCK, KV_HEADS, group_size, HEAD_DIM)

    def attend_block(block_args):
        block_id, q_block = block_args
        scores = jnp.einsum('qkgd,tkd->qkgt', q_block.astype(jnp.float32), k_float) * score_scale
        query_pos = block_id * Q_BLOCK + jnp.arange(Q_BLOCK)
        allowed = key_pos[None, :] <= query_pos[:, None]
        scores = jnp.where(allowed[:, None, None, :], scores, -jnp.inf)
        row_max = jnp.max(scores, axis=-1, keepdims=True)
        weights = jnp.exp(scores - row_max)
        row_sum = jnp.sum(weights, axis=-1, keepdims=True)
        probs = weights.astype(jnp.bfloat16).astype(jnp.float32)
        numer = jnp.einsum('qkgt,tkd->qkgd', probs, v_float)
        return (numer / row_sum).astype(jnp.bfloat16)

    attn = lax.map(attend_block, (jnp.arange(TOKENS // Q_BLOCK), q_blocks))
    attn_flat = attn.reshape(TOKENS, HEADS * HEAD_DIM)
    attn_out = jnp.dot(attn_flat, w_o, preferred_element_type=jnp.float32)
    gate_proj = jnp.dot(normed, w_gate, preferred_element_type=jnp.float32).astype(jnp.bfloat16)
    up_proj = jnp.dot(normed, w_up, preferred_element_type=jnp.float32).astype(jnp.bfloat16)
    mlp_act = (jax.nn.silu(gate_proj.astype(jnp.float32)) * up_proj.astype(jnp.float32)).astype(jnp.bfloat16)
    mlp_out = jnp.dot(mlp_act, w_down, preferred_element_type=jnp.float32)
    hidden_out = (hidden.astype(jnp.float32) + attn_out + mlp_out).astype(jnp.bfloat16)
    return (hidden_out, k_cache, v_cache)
```

```python
import functools

import jax
import jax.numpy as jnp
import numpy as np
from jax import lax
from jax.experimental import pallas as pl
from jax.experimental.pallas import tpu as pltpu
from jax.sharding import PartitionSpec as P

HEAD_DIM = 128
ROPE_BASE = 4000000
LN_EPS = 1e-5
D = 3072
T = 32
R = 128
QW = 1536
KW = 512
GW = 384
FF = 1024
FFT = 4096
NO = 768
KC = 4
NEG = -1e30
F32 = jnp.float32
BF16 = jnp.bfloat16


def mm(a, b):
    return jnp.dot(a, b, preferred_element_type=F32)


def rope(x, cos, sin, even):
    left = pltpu.roll(x, 127, 1)
    right = pltpu.roll(x, 1, 1)
    return (x * cos + jnp.where(even, -left, right) * sin).astype(BF16)


def kernel(hid, pos, gain, invf, wq, wk, wv, wo, wg, wu, wd,
           out_h, out_k, out_v,
           wq_s, wk_s, wv_s, wo_s, wg_s, wu_s, wd_s,
           h_all, accq, acck, accv, q_my, q_all, kv_my, kv_all, s_s, o_my, o_cat,
           a_all, m_my, m_cat, m_oth, p_my, p_oth,
           w_sem, hs, hr, fs, fr, qs, qr, ks, kr, k1s, k1r, v1s, v1r, k2s, k2r, v2s, v2r,
           as_, ar, os_, orr, ms, mr, ds_, dr):
    tp = lax.axis_index('tp')
    cp = lax.axis_index('cp')
    x = lax.rem(cp, 4)
    y = lax.rem(cp // 4, 4)
    z = cp // 16

    def xp(d):
        return tp, z * 16 + y * 4 + lax.rem(x + d, 4)

    def yp(d):
        return tp, z * 16 + lax.rem(y + d, 4) * 4 + x

    def zp(d):
        return tp, lax.rem(z + d, 4) * 16 + y * 4 + x

    mate = (1 - tp, cp)

    def rcopy(src, dst, ss, rs, dev):
        return pltpu.make_async_remote_copy(
            src_ref=src, dst_ref=dst, send_sem=ss, recv_sem=rs,
            device_id={'tp': dev[0], 'cp': dev[1]}, device_id_type=pl.DeviceIdType.MESH)

    kc = D // KC
    wcp = []
    for i in range(KC):
        rows = pl.ds(i * kc, kc)
        for n, (src, dst) in enumerate(((wq, wq_s), (wk, wk_s), (wv, wv_s))):
            wcp.append(pltpu.make_async_copy(src.at[rows], dst.at[rows], w_sem.at[3 * i + n]))
    fcol = pl.ds(pl.multiple_of(x * FF, FF), FF)
    ncol = pl.ds(pl.multiple_of(x * NO, NO), NO)
    cg = pltpu.make_async_copy(wg.at[:, fcol], wg_s, w_sem.at[12])
    cu = pltpu.make_async_copy(wu.at[:, fcol], wu_s, w_sem.at[13])
    cd = pltpu.make_async_copy(wd.at[:, ncol], wd_s, w_sem.at[14])
    co = pltpu.make_async_copy(wo, wo_s, w_sem.at[15])
    for c in wcp + [cg, cu, cd, co]:
        c.start()

    barrier = pltpu.get_barrier_semaphore()
    peers = [f(d) for f in (xp, yp, zp) for d in (1, 2, 3)] + [mate]
    for dev in peers:
        pl.semaphore_signal(barrier, inc=1, device_id={'tp': dev[0], 'cp': dev[1]}, device_id_type=pl.DeviceIdType.MESH)

    hf = hid[...].astype(F32)
    mean = jnp.sum(hf, axis=-1, keepdims=True) * (1.0 / D)
    cen = hf - mean
    var = jnp.sum(cen * cen, axis=-1, keepdims=True) * (1.0 / D)
    h = (cen * lax.rsqrt(var + LN_EPS) * gain[...].astype(F32)).astype(BF16)
    myrows = pl.ds(pl.multiple_of(x * T, T), T)
    h_all[myrows, :] = h

    pl.semaphore_wait(barrier, len(peers))
    hcol = pl.ds(pl.multiple_of(tp * QW, QW), QW)
    hcp = []
    for d in (1, 3, 2):
        c = rcopy(h_all.at[myrows, hcol], h_all.at[myrows, hcol], hs.at[d - 1], hr.at[d - 1], xp(d))
        c.start()
        hcp.append((d, c))

    diag = lax.broadcasted_iota(jnp.int32, (T, T), 0) == lax.broadcasted_iota(jnp.int32, (T, T), 1)
    posf = jnp.sum(jnp.where(diag, jnp.broadcast_to(pos[...].astype(F32), (T, T)), 0.0), axis=1, keepdims=True)
    ang = posf * invf[...]
    cos = jnp.cos(ang)
    sin = jnp.sin(ang)
    even = lax.rem(lax.broadcasted_iota(jnp.int32, (T, HEAD_DIM), 1), 2) == 0

    for i in range(KC):
        rows = slice(i * kc, (i + 1) * kc)
        hi = h[:, rows]
        for n, (w, acc) in enumerate(((wq_s, accq), (wk_s, acck), (wv_s, accv))):
            wcp[3 * i + n].wait()
            part = mm(hi, w[rows, :])
            if i == 0:
                acc[...] = part
            else:
                acc[...] += part

    for j in range(4):
        cols = slice(j * HEAD_DIM, (j + 1) * HEAD_DIM)
        kj = rope(acck[:, cols].astype(BF16).astype(F32), cos, sin, even)
        vj = accv[:, cols].astype(BF16)
        kv_my[j, 0] = kj
        kv_my[j, 1] = vj
        out_k[:, cols] = kj
        out_v[:, cols] = vj
    kcp = []
    for d in (1, 2, 3):
        dst = lax.rem(x + d, 4)
        c = rcopy(kv_my.at[dst], kv_all.at[:, z, y, myrows], ks.at[d - 1], kr.at[d - 1], xp(d))
        c.start()
        kcp.append(c)
    kv_all[:, z, y, myrows, :] = kv_my[x]
    for j in range(12):
        cols = slice(j * HEAD_DIM, (j + 1) * HEAD_DIM)
        q_my[j // 3, :, (j % 3) * HEAD_DIM:(j % 3 + 1) * HEAD_DIM] = rope(
            accq[:, cols].astype(BF16).astype(F32), cos, sin, even)
    qcp = []
    for d in (1, 2, 3):
        dst = lax.rem(x + d, 4)
        c = rcopy(q_my.at[dst], q_all.at[myrows], qs.at[d - 1], qr.at[d - 1], xp(d))
        c.start()
        qcp.append(c)
    q_all[myrows, :] = q_my[x]

    fcp = []
    for d, c in hcp:
        c.wait_recv()
        frm = pl.ds(pl.multiple_of(lax.rem(x + 4 - d, 4) * T, T), T)
        f = rcopy(h_all.at[frm, hcol], h_all.at[frm, hcol], fs.at[d - 1], fr.at[d - 1], mate)
        f.start()
        fcp.append(f)

    for c in kcp:
        c.wait_recv()
    cps1 = []
    for d in (1, 3, 2):
        a = rcopy(kv_all.at[0, z, y], kv_all.at[0, z, y], k1s.at[d - 1], k1r.at[d - 1], yp(d))
        b = rcopy(kv_all.at[1, z, y], kv_all.at[1, z, y], v1s.at[d - 1], v1r.at[d - 1], zp(d))
        a.start()
        b.start()
        cps1 += [a, b]

    for f in fcp:
        f.wait_recv()

    def gate_up(i):
        cols = slice(i * 512, (i + 1) * 512)
        g = mm(h_all[...], wg_s[:, cols]).astype(BF16).astype(F32)
        u = mm(h_all[...], wu_s[:, cols]).astype(BF16).astype(F32)
        act = (g * jax.nn.sigmoid(g) * u).astype(BF16)
        a_all[x, :, cols] = act
        res = []
        for d in (1, 3, 2):
            c = rcopy(a_all.at[x, :, cols], a_all.at[x, :, cols],
                      as_.at[3 * i + d - 1], ar.at[3 * i + d - 1], xp(d))
            c.start()
            res.append(c)
        return res

    cg.wait()
    cu.wait()
    acp = gate_up(0)

    for c in cps1:
        c.wait_recv()
    cps2 = []
    for d in (1, 3, 2):
        a = rcopy(kv_all.at[0, z], kv_all.at[0, z], k2s.at[d - 1], k2r.at[d - 1], zp(d))
        b = rcopy(kv_all.at[1, :, y], kv_all.at[1, :, y], v2s.at[d - 1], v2r.at[d - 1], yp(d))
        a.start()
        b.start()
        cps2 += [a, b]

    acp += gate_up(1)

    for c in qcp:
        c.wait_recv()
    for c in cps2:
        c.wait_recv()

    q3 = jnp.concatenate([q_all[:, g * HEAD_DIM:(g + 1) * HEAD_DIM] for g in range(3)], axis=0)
    base = (z * 4 + y) * R
    row_tok = base + jnp.concatenate([lax.broadcasted_iota(jnp.int32, (R, 512), 0)] * 3, axis=0)
    col_tok = lax.broadcasted_iota(jnp.int32, (3 * R, 512), 1)

    def score_step(zz, row_max):
        kz = kv_all[0, zz].reshape(512, HEAD_DIM)
        s = lax.dot_general(q3, kz, (((1,), (1,)), ((), ())), preferred_element_type=F32) * (HEAD_DIM ** -0.5)
        s = jnp.where(col_tok + zz * 512 <= row_tok, s, NEG)
        s_s[zz] = s
        return jnp.maximum(row_max, jnp.max(s, axis=-1, keepdims=True))

    row_max = lax.fori_loop(0, z + 1, score_step, jnp.full((3 * R, 1), NEG, F32))

    def value_step(zz, state):
        row_sum, accum = state
        e = jnp.exp(s_s[zz] - row_max)
        vz = kv_all[1, zz].reshape(512, HEAD_DIM)
        return row_sum + jnp.sum(e, axis=-1, keepdims=True), accum + mm(e.astype(BF16), vz)

    row_sum, accum = lax.fori_loop(
        0, z + 1, value_step, (jnp.zeros((3 * R, 1), F32), jnp.zeros((3 * R, HEAD_DIM), F32)))
    o3 = (accum / row_sum).astype(BF16)
    for g in range(3):
        o_my[:, g * HEAD_DIM:(g + 1) * HEAD_DIM] = o3[g * R:(g + 1) * R]
    ocol = pl.ds(pl.multiple_of(x * GW, GW), GW)
    ocp = []
    for d in (1, 2, 3):
        rows = pl.ds(pl.multiple_of(lax.rem(x + d, 4) * T, T), T)
        c = rcopy(o_my.at[rows], o_cat.at[:, ocol], os_.at[d - 1], orr.at[d - 1], xp(d))
        c.start()
        ocp.append(c)
    o_cat[:, ocol] = o_my[myrows, :]

    for c in acp:
        c.wait_recv()
    cd.wait()
    macc = mm(a_all[0], wd_s[0:FF, :])
    for i in range(1, 4):
        macc = macc + mm(a_all[i], wd_s[i * FF:(i + 1) * FF, :])
    m_my[...] = macc.astype(BF16)
    mcp = []
    for d in (1, 2, 3):
        rows = pl.ds(pl.multiple_of(lax.rem(x + d, 4) * T, T), T)
        c = rcopy(m_my.at[rows], m_cat.at[:, ncol], ms.at[d - 1], mr.at[d - 1], xp(d))
        c.start()
        mcp.append(c)
    m_cat[:, ncol] = m_my[myrows, :]

    for c in ocp:
        c.wait_recv()
    co.wait()
    p_my[...] = mm(o_cat[...], wo_s[...]).astype(BF16)
    dp_ = rcopy(p_my, p_oth, ds_.at[0], dr.at[0], mate)
    dp_.start()
    for c in mcp:
        c.wait_recv()
    dm = rcopy(m_cat, m_oth, ds_.at[1], dr.at[1], mate)
    dm.start()
    dp_.wait_recv()
    attn = p_my[...].astype(F32) + p_oth[...].astype(F32)
    dm.wait_recv()
    out_h[...] = (hid[...].astype(F32) + attn + (m_cat[...].astype(F32) + m_oth[...].astype(F32))).astype(BF16)

    for c in [c for _, c in hcp] + fcp + qcp + kcp + cps1 + cps2 + acp + ocp + mcp + [dp_, dm]:
        c.wait_send()


def solution(mesh):
    inv = (1.0 / (np.float32(ROPE_BASE) ** (np.arange(0, HEAD_DIM, 2, dtype=np.float32) / np.float32(HEAD_DIM)))).astype(np.float32)
    inv = np.repeat(inv, 2).reshape(1, HEAD_DIM)

    def local_layer(hidden, positions, ln_gain, w_q, w_k, w_v, w_o, w_gate, w_up, w_down):
        vm = pl.BlockSpec(memory_space=pltpu.VMEM)
        hb = pl.BlockSpec(memory_space=pl.ANY)
        dma = pltpu.SemaphoreType.DMA
        V = pltpu.VMEM
        scratch = [
            V((D, QW), BF16), V((D, KW), BF16), V((D, KW), BF16), V((QW, D), BF16),
            V((D, FF), BF16), V((D, FF), BF16), V((FFT, NO), BF16),
            V((R, D), BF16), V((T, QW), F32), V((T, KW), F32), V((T, KW), F32),
            V((4, T, GW), BF16), V((R, GW), BF16), V((4, 2, T, HEAD_DIM), BF16),
            V((2, 4, 4, R, HEAD_DIM), BF16), V((4, 3 * R, 512), F32), V((R, GW), BF16), V((T, QW), BF16),
            V((4, R, FF), BF16), V((R, NO), BF16), V((T, D), BF16), V((T, D), BF16), V((T, D), BF16), V((T, D), BF16),
            dma((16,)), dma((3,)), dma((3,)), dma((3,)), dma((3,)), dma((3,)), dma((3,)), dma((3,)), dma((3,)),
            dma((3,)), dma((3,)), dma((3,)), dma((3,)), dma((3,)), dma((3,)), dma((3,)), dma((3,)),
            dma((6,)), dma((6,)), dma((3,)), dma((3,)), dma((3,)), dma((3,)), dma((2,)), dma((2,)),
        ]
        out_h, out_k, out_v = pl.pallas_call(
            kernel,
            name='layer',
            out_shape=(jax.ShapeDtypeStruct((T, D), BF16), jax.ShapeDtypeStruct((T, KW), BF16), jax.ShapeDtypeStruct((T, KW), BF16)),
            in_specs=[vm, vm, vm, vm] + [hb] * 7,
            out_specs=(vm, vm, vm),
            scratch_shapes=scratch,
            compiler_params=pltpu.CompilerParams(collective_id=0, has_side_effects=True, vmem_limit_bytes=67043328),
        )(hidden, positions.reshape(1, T), ln_gain.reshape(1, D), jnp.asarray(inv), w_q, w_k, w_v, w_o, w_gate, w_up, w_down)
        return out_h, out_k.reshape(T, 4, HEAD_DIM), out_v.reshape(T, 4, HEAD_DIM)

    row_spec = P(('dp', 'cp'), None)
    col_spec = P(None, 'tp')
    cache_spec = P(('dp', 'cp'), 'tp', None)
    in_specs = (row_spec, P(('dp', 'cp')), P(None), col_spec, col_spec, col_spec, P('tp', None), col_spec, col_spec, P('tp', None))
    return jax.shard_map(local_layer, mesh=mesh, in_specs=in_specs, out_specs=(row_spec, cache_spec, cache_spec), check_vma=False)
```

```python
import jax
import jax.numpy as jnp
import numpy as np
from jax import lax
from jax.experimental import pallas as pl
from jax.experimental.pallas import tpu as pltpu
from jax.sharding import PartitionSpec as P

HEAD_DIM = 128
ROPE_BASE = 4000000
LN_EPS = 1e-5
D = 3072
T = 32
R = 128
QW = 1536
KW = 512
GW = 384
FF = 1024
FFT = 4096
KC = 4
NEG = -1e30
F32 = jnp.float32
BF16 = jnp.bfloat16
RING = (1, 3, 2)
KUP = (0, 1)
VUP = (1,)


def mm(a, b):
    return jnp.dot(a, b, preferred_element_type=F32)


def rope(x, cos, sin, even):
    left = pltpu.roll(x, 127, 1)
    right = pltpu.roll(x, 1, 1)
    return (x * cos + jnp.where(even, -left, right) * sin).astype(BF16)


def kernel(hid, pos, gain, invf, wq, wk, wv, wo, wg, wu, wd,
           out_h, out_k, out_v,
           hid_s, pos_s, gain_s, inv_s,
           wq_s, wk_s, wv_s, wo_s, wg_s, wu_s, wda_s, wdx_s,
           h_all, accq, acck, accv, kx, vx, q_my, q_all, kv_my, kv_all,
           mx_s, sum_s, acc_s, o_my, o_cat,
           a_my, a_cat, m_my, m_oth, p_my, p_oth,
           i_sem, w_sem, hs, hr, fs, fr, qs, qr, ks, kr, k1s, k1r, v1s, v1r, k2s, k2r, v2s, v2r,
           as_, ar, os_, orr, ds_, dr):
    scope = []

    def phase(name):
        if scope:
            scope.pop().__exit__(None, None, None)
        if name:
            scope.append(jax.named_scope(name))
            scope[0].__enter__()

    phase('start')
    tp = lax.axis_index('tp')
    cp = lax.axis_index('cp')
    x = lax.rem(cp, 4)
    y = lax.rem(cp // 4, 4)
    z = cp // 16

    def xp(d):
        return tp, z * 16 + y * 4 + lax.rem(x + d, 4)

    def yp(d):
        return tp, z * 16 + lax.rem(y + d, 4) * 4 + x

    def zp(d):
        return tp, lax.rem(z + d, 4) * 16 + y * 4 + x

    mate = (1 - tp, cp)

    def rcopy(src, dst, ss, rs, dev):
        return pltpu.make_async_remote_copy(
            src_ref=src, dst_ref=dst, send_sem=ss, recv_sem=rs,
            device_id={'tp': dev[0], 'cp': dev[1]}, device_id_type=pl.DeviceIdType.MESH)

    small = [pltpu.make_async_copy(a, b, i_sem.at[i])
             for i, (a, b) in enumerate(((hid, hid_s), (gain, gain_s), (pos, pos_s), (invf, inv_s)))]
    for c in small:
        c.start()
    kc = D // KC
    wcp = []
    for i in range(KC):
        rows = pl.ds(i * kc, kc)
        for n, (src, dst) in enumerate(((wq, wq_s), (wk, wk_s), (wv, wv_s))):
            wcp.append(pltpu.make_async_copy(src.at[rows], dst.at[rows], w_sem.at[3 * i + n]))
    fcol = pl.ds(pl.multiple_of(x * FF, FF), FF)
    cg = pltpu.make_async_copy(wg.at[:, fcol], wg_s, w_sem.at[12])
    cu = pltpu.make_async_copy(wu.at[:, fcol], wu_s, w_sem.at[13])
    cda = pltpu.make_async_copy(wd.at[pl.ds(0, FF)], wda_s, w_sem.at[14])
    low = pl.ds(FF, D)
    cdx = pltpu.make_async_copy(wd.at[low, pl.ds(QW + 2 * KW, KW)], wdx_s, w_sem.at[15])
    co = pltpu.make_async_copy(wo, wo_s, w_sem.at[16])
    cdq = pltpu.make_async_copy(wd.at[low, pl.ds(0, QW)], wq_s, w_sem.at[17])
    cdk = pltpu.make_async_copy(wd.at[low, pl.ds(QW, KW)], wk_s, w_sem.at[18])
    cdv = pltpu.make_async_copy(wd.at[low, pl.ds(QW + KW, KW)], wv_s, w_sem.at[19])
    for c in wcp[:3]:
        c.start()

    barrier = pltpu.get_barrier_semaphore()
    peers = [f(d) for f in (xp, yp, zp) for d in (1, 2, 3)] + [mate]
    for dev in peers:
        pl.semaphore_signal(barrier, inc=1, device_id={'tp': dev[0], 'cp': dev[1]}, device_id_type=pl.DeviceIdType.MESH)

    for yy in range(4):
        @pl.when(yy > y)
        def _(yy=yy):
            kv_all[1, z, yy] = jnp.zeros((R, HEAD_DIM), BF16)

        @pl.when(jnp.logical_and(yy > y, z == 3))
        def _(yy=yy):
            kv_all[0, z, yy] = jnp.zeros((R, HEAD_DIM), BF16)

    phase('ln')
    for c in small:
        c.wait()
    for c in wcp[3:] + [cg, cu, cda, cdx]:
        c.start()
    hf = hid_s[...].astype(F32)
    mean = jnp.sum(hf, axis=-1, keepdims=True) * (1.0 / D)
    cen = hf - mean
    var = jnp.sum(cen * cen, axis=-1, keepdims=True) * (1.0 / D)
    scaled = cen * lax.rsqrt(var + LN_EPS)
    gf = gain_s[...].astype(F32)
    myrows = pl.ds(pl.multiple_of(x * T, T), T)
    for i in range(D // HEAD_DIM):
        cols = slice(i * HEAD_DIM, (i + 1) * HEAD_DIM)
        h_all[myrows, cols] = (scaled[:, cols] * gf[i:i + 1]).astype(BF16)

    phase('tables')
    diag = lax.broadcasted_iota(jnp.int32, (T, T), 0) == lax.broadcasted_iota(jnp.int32, (T, T), 1)
    posf = jnp.sum(jnp.where(diag, jnp.broadcast_to(pos_s[...].astype(F32), (T, T)), 0.0), axis=1, keepdims=True)
    ang = posf * inv_s[...]
    cos = jnp.cos(ang)
    sin = jnp.sin(ang)
    even = lax.rem(lax.broadcasted_iota(jnp.int32, (T, HEAD_DIM), 1), 2) == 0

    def qkv(i):
        rows = slice(i * kc, (i + 1) * kc)
        hi = h_all[myrows, rows]
        for n, (w, acc) in enumerate(((wq_s, accq), (wk_s, acck), (wv_s, accv))):
            wcp[3 * i + n].wait()
            part = mm(hi, w[rows, :])
            if i == 0:
                acc[...] = part
            else:
                acc[...] += part

    hcol = pl.ds(pl.multiple_of(tp * QW, QW), QW)
    hhalf = [pl.ds(pl.multiple_of(tp * QW + n * (QW // 2), QW // 2), QW // 2) for n in range(2)]

    def hblock(frm, cols, n, dev, ss, rs):
        rows = pl.ds(pl.multiple_of(lax.rem(frm, 4) * T, T), T)
        b = h_all.at[rows, cols]
        return rcopy(b, b, ss.at[n], rs.at[n], dev)

    hcp = [hblock(x, hcol, 0, xp(1), hs, hr), hblock(x, hcol, 1, xp(3), hs, hr),
           hblock(x + 3, hhalf[0], 2, xp(1), hs, hr), hblock(x + 1, hhalf[1], 3, xp(3), hs, hr)]
    fcp = [hblock(x + 3, hcol, 0, mate, fs, fr), hblock(x + 1, hcol, 1, mate, fs, fr),
           hblock(x + 2, hhalf[0], 2, mate, fs, fr), hblock(x + 2, hhalf[1], 3, mate, fs, fr)]

    phase('qkv0')
    qkv(0)
    qkv(1)
    phase('barrier')
    pl.semaphore_wait(barrier, len(peers))
    hcp[0].start()
    hcp[1].start()
    phase('qkv1')
    qkv(2)
    qkv(3)
    for c in (cdq, cdk, cdv, co):
        c.start()

    phase('rope')
    for j in range(4):
        cols = slice(j * HEAD_DIM, (j + 1) * HEAD_DIM)
        kj = rope(acck[:, cols].astype(BF16).astype(F32), cos, sin, even)
        vj = accv[:, cols].astype(BF16)
        kv_my[j, 0] = kj
        kv_my[j, 1] = vj
        kx[pl.ds(j, T, stride=4), :] = kj.astype(F32)
        vx[pl.ds(j, T, stride=4), :] = vj.astype(F32)
    kcp = []
    for d in RING:
        dst = lax.rem(x + d, 4)
        c = rcopy(kv_my.at[dst], kv_all.at[:, z, y, myrows], ks.at[d - 1], kr.at[d - 1], xp(d))
        c.start()
        kcp.append(c)
    kv_all[:, z, y, myrows, :] = kv_my[x]
    for j in range(12):
        cols = slice(j * HEAD_DIM, (j + 1) * HEAD_DIM)
        q_my[j // 3, :, (j % 3) * HEAD_DIM:(j % 3 + 1) * HEAD_DIM] = rope(
            accq[:, cols].astype(BF16).astype(F32), cos, sin, even)
    qcp = []
    for d in RING:
        dst = lax.rem(x + d, 4)
        c = rcopy(q_my.at[dst], q_all.at[myrows], qs.at[d - 1], qr.at[d - 1], xp(d))
        c.start()
        qcp.append(c)
    q_all[myrows, :] = q_my[x]

    phase('hwait')
    for n in range(2):
        hcp[n].wait_recv()
        hcp[n + 2].start()
        fcp[n].start()

    def k1(d):
        b = kv_all.at[0, z, y]
        return rcopy(b, b, k1s.at[d - 1], k1r.at[d - 1], yp(d))

    def v1(d):
        b = kv_all.at[1, z, y]
        return rcopy(b, b, v1s.at[d - 1], v1r.at[d - 1], zp(d))

    def k2(dy, dz):
        row = {1: z, 3: z, 2: lax.rem(z + 3, 4) if dy in KUP else lax.rem(z + 1, 4)}[dz]
        b = kv_all.at[0, row, lax.rem(y + 4 - dy, 4)]
        dev = zp({1: 1, 3: 3, 2: 1 if dy in KUP else 3}[dz])
        return rcopy(b, b, k2s.at[3 * dy + dz - 1], k2r.at[3 * dy + dz - 1], dev)

    def v2(dz, dy):
        far = dy == 2 and dz > 0
        col = y if not far else lax.rem(y + (3 if dz in VUP else 1), 4)
        b = kv_all.at[1, lax.rem(z + 4 - dz, 4), col]
        dev = yp(dy if not far else (1 if dz in VUP else 3))
        return rcopy(b, b, v2s.at[3 * dz + dy - 1], v2r.at[3 * dz + dy - 1], dev)

    def k2_out(dy, dz):
        if dz == 1:
            return z <= 2
        if dz == 3:
            return z == 0 if dy in KUP else z <= 1
        return jnp.logical_or(z == 1, z == 2) if dy in KUP else jnp.logical_or(z == 3, z == 0)

    def k2_in(dy, dz):
        if dz == 1:
            return z >= 1
        if dz == 3:
            return z == 3 if dy in KUP else jnp.logical_or(z == 3, z == 0)
        return z >= 2

    k1_out = {d: jnp.logical_or(y + d <= 3, z < 3) for d in RING}
    k1_in = {d: jnp.logical_or(y >= d, z < 3) for d in RING}
    z_out = {d: z + d <= 3 for d in RING}
    z_in = {d: z >= d for d in RING}
    v20_out = {d: y + d <= 3 for d in RING}
    v20_in = {d: y >= d for d in RING}

    def when(cond, fn):
        pl.when(cond)(lambda: fn())

    phase('kvx')
    for c in kcp:
        c.wait_recv()
    for d in RING:
        when(k1_out[d], lambda d=d: k1(d).start())
        when(z_out[d], lambda d=d: v1(d).start())
    for d in RING:
        if d != 2:
            when(k2_out(0, d), lambda d=d: k2(0, d).start())
        when(v20_out[d], lambda d=d: v2(0, d).start())

    phase('hwait2')
    for n in (2, 3):
        hcp[n].wait_recv()
        fcp[n].start()
    for f in fcp:
        f.wait_recv()
    phase('guwait')
    cg.wait()
    cu.wait()

    def acopy(i, d):
        rows = pl.ds(pl.multiple_of(lax.rem(x + d, 4) * T, T), T)
        cols = pl.ds(pl.multiple_of(x * FF + i * 512, 512), 512)
        return rcopy(a_my.at[rows, pl.ds(i * 512, 512)], a_cat.at[:, cols],
                     as_.at[3 * i + d - 1], ar.at[3 * i + d - 1], xp(d))

    def gate_up(i):
        cols = slice(i * 512, (i + 1) * 512)
        g = mm(h_all[...], wg_s[:, cols]).astype(BF16).astype(F32)
        u = mm(h_all[...], wu_s[:, cols]).astype(BF16).astype(F32)
        a_my[:, cols] = (g * jax.nn.sigmoid(g) * u).astype(BF16)
        for d in RING:
            acopy(i, d).start()
        a_cat[:, pl.ds(pl.multiple_of(x * FF + i * 512, 512), 512)] = a_my[myrows, cols]

    phase('gu0')
    gate_up(0)

    phase('k1wait')
    for d in RING:
        when(k1_in[d], lambda d=d: k1(d).wait_recv())
        for dz in (1, 3):
            when(k2_out(d, dz), lambda d=d, dz=dz: k2(d, dz).start())

        @pl.when(z_in[d])
        def _(d=d):
            v1(d).wait_recv()
            for dy in (1, 3):
                v2(d, dy).start()

    phase('gu1')
    gate_up(1)

    phase('qwait')
    for c in qcp:
        c.wait_recv()
    q3 = jnp.concatenate([q_all[:, g * HEAD_DIM:(g + 1) * HEAD_DIM] for g in range(3)], axis=0)

    def scores(zz):
        kz = kv_all[0, zz].reshape(512, HEAD_DIM)
        return lax.dot_general(q3, kz, (((1,), (1,)), ((), ())), preferred_element_type=F32) * (HEAD_DIM ** -0.5)

    for d in RING:
        when(v20_in[d], lambda d=d: v2(0, d).wait_recv())
    phase('row0')
    row_tok = y * R + jnp.concatenate([lax.broadcasted_iota(jnp.int32, (R, 512), 0)] * 3, axis=0)
    col_tok = lax.broadcasted_iota(jnp.int32, (3 * R, 512), 1)
    s = jnp.where(col_tok <= row_tok, scores(z), NEG)
    m0 = jnp.max(s, axis=-1, keepdims=True)
    e = jnp.exp(s - m0)
    mx_s[...] = m0
    sum_s[...] = jnp.sum(e, axis=-1, keepdims=True)
    acc_s[...] = mm(e.astype(BF16), kv_all[1, z].reshape(512, HEAD_DIM))

    phase('relay')
    for i, dy in enumerate((0, 1, 3, 2)):
        for dz, up in ((1, True), (3, False)):
            when(k2_in(dy, dz), lambda dy=dy, dz=dz: k2(dy, dz).wait_recv())
            if (dy in KUP) == up:
                when(k2_out(dy, 2), lambda dy=dy: k2(dy, 2).start())
        if i:
            dz = dy

            @pl.when(z_in[dz])
            def _(dz=dz):
                for dd, up in ((1, True), (3, False)):
                    v2(dz, dd).wait_recv()
                    if (dz in VUP) == up:
                        v2(dz, 2).start()

    for dz in RING:
        phase(f'row{dz}')

        @pl.when(z_in[dz])
        def _(dz=dz):
            zz = z - dz
            if dz == 2:
                for dy in range(4):
                    k2(dy, 2).wait_recv()
            v2(dz, 2).wait_recv()
            s = scores(zz)
            m_old = mx_s[...]
            m_new = jnp.maximum(m_old, jnp.max(s, axis=-1, keepdims=True))
            e = jnp.exp(s - m_new)
            f = jnp.exp(m_old - m_new)
            mx_s[...] = m_new
            sum_s[...] = sum_s[...] * f + jnp.sum(e, axis=-1, keepdims=True)
            acc_s[...] = acc_s[...] * f + mm(e.astype(BF16), kv_all[1, zz].reshape(512, HEAD_DIM))

    phase('osend')
    o3 = (acc_s[...] / sum_s[...]).astype(BF16)
    for g in range(3):
        o_my[:, g * HEAD_DIM:(g + 1) * HEAD_DIM] = o3[g * R:(g + 1) * R]
    ocol = pl.ds(pl.multiple_of(x * GW, GW), GW)
    ocp = []
    for d in RING:
        rows = pl.ds(pl.multiple_of(lax.rem(x + d, 4) * T, T), T)
        c = rcopy(o_my.at[rows], o_cat.at[:, ocol], os_.at[d - 1], orr.at[d - 1], xp(d))
        c.start()
        ocp.append(c)
    o_cat[:, ocol] = o_my[myrows, :]
    out_k[...] = kx[...].astype(BF16)
    out_v[...] = vx[...].astype(BF16)

    phase('await')
    for i in range(2):
        for d in RING:
            acopy(i, d).wait_recv()
    phase('wdwait')
    for c in (cda, cdx, cdq, cdk, cdv):
        c.wait()
    phase('down')
    a_lo = a_cat[:, 0:FF]
    a_hi = a_cat[:, FF:]
    at = 0
    for w in (wq_s, wk_s, wv_s, wdx_s):
        n = w.shape[1]
        m_my[:, at:at + n] = (mm(a_hi, w[...]) + mm(a_lo, wda_s[:, at:at + n])).astype(BF16)
        at += n
    dm = rcopy(m_my, m_oth, ds_.at[1], dr.at[1], mate)
    dm.start()

    phase('owait')
    for c in ocp:
        c.wait_recv()
    co.wait()
    phase('wo')
    p_my[...] = mm(o_cat[...], wo_s[...]).astype(BF16)
    dp_ = rcopy(p_my, p_oth, ds_.at[0], dr.at[0], mate)
    dp_.start()
    phase('final')
    dm.wait_recv()
    rest = hid_s[...].astype(F32) + (m_my[...].astype(F32) + m_oth[...].astype(F32))
    dp_.wait_recv()
    out_h[...] = (rest + (p_my[...].astype(F32) + p_oth[...].astype(F32))).astype(BF16)

    phase('drain')
    for c in hcp + fcp + qcp + kcp + ocp + [dm, dp_]:
        c.wait_send()
    for i in range(2):
        for d in RING:
            acopy(i, d).wait_send()
    for d in RING:
        when(k1_out[d], lambda d=d: k1(d).wait_send())
        when(v20_out[d], lambda d=d: v2(0, d).wait_send())

        for dy in range(4):
            when(k2_out(dy, d), lambda d=d, dy=dy: k2(dy, d).wait_send())
        when(z_out[d], lambda d=d: v1(d).wait_send())

        @pl.when(z_in[d])
        def _(d=d):
            for dy in RING:
                v2(d, dy).wait_send()
    phase(None)


def emit(h, k, v, out_h, out_k, out_v, sem):
    cps = [pltpu.make_async_copy(a, b, sem.at[i]) for i, (a, b) in enumerate(((h, out_h), (k, out_k), (v, out_v)))]
    for c in cps:
        c.start()
    for c in cps:
        c.wait()


def solution(mesh):
    inv = (1.0 / (np.float32(ROPE_BASE) ** (np.arange(0, HEAD_DIM, 2, dtype=np.float32) / np.float32(HEAD_DIM)))).astype(np.float32)
    inv = np.repeat(inv, 2).reshape(1, HEAD_DIM)

    def local_layer(hidden, positions, ln_gain, w_q, w_k, w_v, w_o, w_gate, w_up, w_down):
        vm = pl.BlockSpec(memory_space=pltpu.VMEM)
        hb = pl.BlockSpec(memory_space=pl.ANY)
        dma = pltpu.SemaphoreType.DMA
        V = pltpu.VMEM
        scratch = [
            V((T, D), BF16), V((1, T), jnp.int32), V((D // HEAD_DIM, HEAD_DIM), BF16), V((1, HEAD_DIM), F32),
            V((D, QW), BF16), V((D, KW), BF16), V((D, KW), BF16), V((QW, D), BF16),
            V((D, FF), BF16), V((D, FF), BF16), V((FF, D), BF16), V((D, KW), BF16),
            V((R, D), BF16), V((T, QW), F32), V((T, KW), F32), V((T, KW), F32), V((R, HEAD_DIM), F32), V((R, HEAD_DIM), F32),
            V((4, T, GW), BF16), V((R, GW), BF16), V((4, 2, T, HEAD_DIM), BF16), V((2, 4, 4, R, HEAD_DIM), BF16),
            V((3 * R, 1), F32), V((3 * R, 1), F32), V((3 * R, HEAD_DIM), F32), V((R, GW), BF16), V((T, QW), BF16),
            V((R, FF), BF16), V((T, FFT), BF16), V((T, D), BF16), V((T, D), BF16), V((T, D), BF16), V((T, D), BF16),
            dma((4,)), dma((20,)), dma((4,)), dma((4,)), dma((4,)), dma((4,)), dma((3,)), dma((3,)), dma((3,)), dma((3,)),
            dma((3,)), dma((3,)), dma((3,)), dma((3,)), dma((12,)), dma((12,)), dma((12,)), dma((12,)),
            dma((6,)), dma((6,)), dma((3,)), dma((3,)), dma((2,)), dma((2,)),
        ]
        outs = (jax.ShapeDtypeStruct((T, D), BF16), jax.ShapeDtypeStruct((R, HEAD_DIM), BF16), jax.ShapeDtypeStruct((R, HEAD_DIM), BF16))
        res = pl.pallas_call(
            kernel,
            name='layer',
            out_shape=tuple(pltpu.VMEM(o.shape, o.dtype) for o in outs),
            in_specs=[hb] * 11,
            out_specs=(vm, vm, vm),
            scratch_shapes=scratch,
            compiler_params=pltpu.CompilerParams(collective_id=0, has_side_effects=True, vmem_limit_bytes=60000000),
        )(hidden, positions.reshape(1, T), ln_gain.reshape(D // HEAD_DIM, HEAD_DIM), jnp.asarray(inv),
          w_q, w_k, w_v, w_o, w_gate, w_up, w_down)
        out_h, out_k, out_v = pl.pallas_call(
            emit,
            name='emit',
            out_shape=outs,
            in_specs=[vm] * 3,
            out_specs=(hb, hb, hb),
            scratch_shapes=[dma((3,))],
        )(*[pltpu.with_memory_space_constraint(r, pltpu.VMEM) for r in res])
        return out_h, out_k.reshape(T, 4, HEAD_DIM), out_v.reshape(T, 4, HEAD_DIM)

    row_spec = P(('dp', 'cp'), None)
    col_spec = P(None, 'tp')
    cache_spec = P(('dp', 'cp'), 'tp', None)
    in_specs = (row_spec, P(('dp', 'cp')), P(None), col_spec, col_spec, col_spec, P('tp', None), col_spec, col_spec, P('tp', None))
    return jax.shard_map(local_layer, mesh=mesh, in_specs=in_specs, out_specs=(row_spec, cache_spec, cache_spec), check_vma=False)
```

```python
import jax
import jax.numpy as jnp
import numpy as np
from jax import lax
from jax.experimental import pallas as pl
from jax.experimental.pallas import tpu as pltpu
from jax.sharding import PartitionSpec as P

HEAD_DIM = 128
ROPE_BASE = 4000000
LN_EPS = 1e-5
D = 3072
T = 32
R = 128
QW = 1536
KW = 512
GW = 384
T2 = 64
FF = 2048
FC = 1024
LO = 1024
FFT = 4096
KC = 4
NG = 512
NEG = -1e30
F32 = jnp.float32
BF16 = jnp.bfloat16
RING = (1, 3, 2)


def mm(a, b):
    return jnp.dot(a, b, preferred_element_type=F32)


def rope(x, cos, sin, even):
    left = pltpu.roll(x, 127, 1)
    right = pltpu.roll(x, 1, 1)
    return (x * cos + jnp.where(even, -left, right) * sin).astype(BF16)


def kernel(hid, pos, gain, invf, wq, wk, wv, wo, wg, wu, wd,
           out_h, out_k, out_v,
           hid_s, pos_s, gain_s, inv_s,
           wq_s, wk_s, wv_s, wg_s, wu_s, wda_s, wdx_s,
           h_all, accq, acck, accv, kx, vx, q_my, q_all, kv_my, kv_all,
           mx_s, sum_s, acc_s, o_my, o_cat,
           a_my, a_cat, m_my, m_oth, p_my, p_oth,
           i_sem, w_sem, hs, hr, fs, fr, qs, qr, ks, kr, k1s, k1r, v1s, v1r, k2s, k2r, v2s, v2r,
           as_, ar, os_, orr, ds_, dr):
    scope = []

    def phase(name):
        if scope:
            scope.pop().__exit__(None, None, None)
        if name:
            scope.append(jax.named_scope(name))
            scope[0].__enter__()

    phase('start')
    tp = lax.axis_index('tp')
    cp = lax.axis_index('cp')
    x = lax.rem(cp, 4)
    y = lax.rem(cp // 4, 4)
    z = cp // 16

    def xp(d):
        return tp, z * 16 + y * 4 + lax.rem(x + d, 4)

    def yp(d):
        return tp, z * 16 + lax.rem(y + d, 4) * 4 + x

    def zp(d):
        return tp, lax.rem(z + d, 4) * 16 + y * 4 + x

    mate = (1 - tp, cp)

    def rcopy(src, dst, ss, rs, dev):
        return pltpu.make_async_remote_copy(
            src_ref=src, dst_ref=dst, send_sem=ss, recv_sem=rs,
            device_id={'tp': dev[0], 'cp': dev[1]}, device_id_type=pl.DeviceIdType.MESH)

    small = [pltpu.make_async_copy(a, b, i_sem.at[i])
             for i, (a, b) in enumerate(((hid, hid_s), (gain, gain_s), (pos, pos_s), (invf, inv_s)))]
    for c in small:
        c.start()
    half = D // 2
    ckv = [pltpu.make_async_copy(src.at[pl.ds(i * half, half)], dst.at[pl.ds(i * half, half)], w_sem.at[2 * i + n])
           for i in range(2) for n, (src, dst) in enumerate(((wk, wk_s), (wv, wv_s)))]
    kc = D // KC
    cwq = [pltpu.make_async_copy(wq.at[pl.ds(i * kc, kc)], wq_s.at[pl.ds(i * kc, kc)], w_sem.at[4 + i]) for i in range(KC)]
    par = lax.rem(x, 2)
    pair = (tp, cp + 1 - 2 * par)
    mine = pl.ds(pl.multiple_of(par * T, T), T)
    theirs = pl.ds(pl.multiple_of((1 - par) * T, T), T)
    hcol = pl.ds(pl.multiple_of(tp * QW, QW), QW)
    cgu = [pltpu.make_async_copy(src.at[:, pl.ds(pl.multiple_of(par * FF + i * FC, FC), FC)],
                                 dst.at[:, pl.ds(i * FC, FC)], w_sem.at[8 + 2 * i + n])
           for i in range(2) for n, (src, dst) in enumerate(((wg, wg_s), (wu, wu_s)))]
    cda = pltpu.make_async_copy(wd.at[pl.ds(0, LO)], wda_s, w_sem.at[16])
    woref = [wg_s.at[pl.ds(0, QW), pl.ds(0, 1024)], wg_s.at[pl.ds(0, QW), pl.ds(1024, 1024)], wg_s.at[pl.ds(QW, QW), pl.ds(0, 1024)]]
    co = [pltpu.make_async_copy(wo.at[:, pl.ds(i * 1024, 1024)], woref[i], w_sem.at[17 + i]) for i in range(3)]
    groups = [(wdx_s.at[:], 5 * NG), (wk_s.at[:], 3 * NG), (wv_s.at[:], 4 * NG)] + [
        (wq_s.at[:, pl.ds(i * NG, NG)], i * NG) for i in range(3)]
    low = pl.ds(LO, D)
    cdw = [pltpu.make_async_copy(wd.at[low, pl.ds(at, NG)], ref, w_sem.at[20 + i]) for i, (ref, at) in enumerate(groups)]
    barrier = pltpu.get_barrier_semaphore()
    peers = [f(d) for f in (xp, yp, zp) for d in (1, 2, 3)] + [mate]
    for dev in peers:
        pl.semaphore_signal(barrier, inc=1, device_id={'tp': dev[0], 'cp': dev[1]}, device_id_type=pl.DeviceIdType.MESH)

    h_all[T2:R, :] = jnp.zeros((R - T2, D), BF16)
    a_cat[T:R, :] = jnp.zeros((R - T, FFT), BF16)
    o_cat[T:R, :] = jnp.zeros((R - T, QW), BF16)

    for yy in range(4):
        @pl.when(yy > y)
        def _(yy=yy):
            kv_all[1, z, yy] = jnp.zeros((R, HEAD_DIM), BF16)

        @pl.when(jnp.logical_and(yy > y, z == 3))
        def _(yy=yy):
            kv_all[0, z, yy] = jnp.zeros((R, HEAD_DIM), BF16)

    phase('ln')
    for c in small:
        c.wait()
    for c in ckv + cwq + cgu + [cda, cdw[0]]:
        c.start()
    hf = hid_s[...].astype(F32)
    mean = jnp.sum(hf, axis=-1, keepdims=True) * (1.0 / D)
    cen = hf - mean
    var = jnp.sum(cen * cen, axis=-1, keepdims=True) * (1.0 / D)
    scaled = cen * lax.rsqrt(var + LN_EPS)
    gf = gain_s[...].astype(F32)
    myrows = pl.ds(pl.multiple_of(x * T, T), T)
    for i in range(D // HEAD_DIM):
        cols = slice(i * HEAD_DIM, (i + 1) * HEAD_DIM)
        h_all[mine, cols] = (scaled[:, cols] * gf[i:i + 1]).astype(BF16)

    hcp = rcopy(h_all.at[mine, hcol], h_all.at[mine, hcol], hs.at[0], hr.at[0], pair)
    fcp = rcopy(h_all.at[theirs, hcol], h_all.at[theirs, hcol], fs.at[0], fr.at[0], mate)
    kcp = {d: rcopy(kv_my.at[lax.rem(x + d, 4)], kv_all.at[:, z, y, myrows], ks.at[d - 1], kr.at[d - 1], xp(d)) for d in RING}

    phase('tables')
    diag = lax.broadcasted_iota(jnp.int32, (T, T), 0) == lax.broadcasted_iota(jnp.int32, (T, T), 1)
    posf = jnp.sum(jnp.where(diag, jnp.broadcast_to(pos_s[...].astype(F32), (T, T)), 0.0), axis=1, keepdims=True)
    ang = posf * inv_s[...]
    cos = jnp.cos(ang)
    sin = jnp.sin(ang)
    even = lax.rem(lax.broadcasted_iota(jnp.int32, (T, HEAD_DIM), 1), 2) == 0

    phase('kvproj')
    for i in range(2):
        rows = slice(i * half, (i + 1) * half)
        for n, (w, acc) in enumerate(((wk_s, acck), (wv_s, accv))):
            ckv[2 * i + n].wait()
            part = mm(h_all[mine, rows], w[rows, :])
            if i == 0:
                acc[...] = part
            else:
                acc[...] += part
    phase('kvrope')
    for j in range(4):
        cols = slice(j * HEAD_DIM, (j + 1) * HEAD_DIM)
        kj = rope(acck[:, cols].astype(BF16).astype(F32), cos, sin, even)
        vj = accv[:, cols].astype(BF16)
        kv_my[j, 0] = kj
        kv_my[j, 1] = vj
        kx[pl.ds(j, T, stride=4), :] = kj.astype(F32)
        vx[pl.ds(j, T, stride=4), :] = vj.astype(F32)
    kv_all[:, z, y, myrows, :] = kv_my[x]

    phase('barrier')
    pl.semaphore_wait(barrier, len(peers))
    for d in RING:
        kcp[d].start()
    hcp.start()

    phase('qproj')
    for i in range(KC):
        rows = slice(i * kc, (i + 1) * kc)
        cwq[i].wait()
        part = mm(h_all[mine, rows], wq_s[rows, :])
        if i == 0:
            accq[...] = part
        else:
            accq[...] += part
    for c in cdw[1:]:
        c.start()

    def k1(d):
        b = kv_all.at[0, z, y]
        return rcopy(b, b, k1s.at[d - 1], k1r.at[d - 1], yp(d))

    def v1(d):
        b = kv_all.at[1, z, y]
        return rcopy(b, b, v1s.at[d - 1], v1r.at[d - 1], zp(d))

    def k2(dy, dz):
        b = kv_all.at[0, z, lax.rem(y + 4 - dy, 4)]
        return rcopy(b, b, k2s.at[3 * dy + dz - 1], k2r.at[3 * dy + dz - 1], zp(dz))

    def v2(dz, dy):
        b = kv_all.at[1, lax.rem(z + 4 - dz, 4), y]
        return rcopy(b, b, v2s.at[3 * dz + dy - 1], v2r.at[3 * dz + dy - 1], yp(dy))

    k1_out = {d: jnp.logical_or(y + d <= 3, z < 3) for d in RING}
    k1_in = {d: jnp.logical_or(y >= d, z < 3) for d in RING}
    z_out = {d: z + d <= 3 for d in RING}
    z_in = {d: z >= d for d in RING}
    v20_out = {d: y + d <= 3 for d in RING}
    v20_in = {d: y >= d for d in RING}

    def when(cond, fn):
        pl.when(cond)(lambda: fn())

    phase('kvx')
    for d in RING:
        kcp[d].wait_recv()
    for d in RING:
        when(k1_out[d], lambda d=d: k1(d).start())
        when(z_out[d], lambda d=d: v1(d).start())
    for d in RING:
        when(z_out[d], lambda d=d: k2(0, d).start())
    for d in RING:
        when(v20_out[d], lambda d=d: v2(0, d).start())

    phase('hwait')
    hcp.wait_recv()
    fcp.start()

    phase('qrope')
    for j in range(12):
        cols = slice(j * HEAD_DIM, (j + 1) * HEAD_DIM)
        q_my[j // 3, :, (j % 3) * HEAD_DIM:(j % 3 + 1) * HEAD_DIM] = rope(
            accq[:, cols].astype(BF16).astype(F32), cos, sin, even)
    qcp = []
    for d in RING:
        dst = lax.rem(x + d, 4)
        c = rcopy(q_my.at[dst], q_all.at[myrows], qs.at[d - 1], qr.at[d - 1], xp(d))
        c.start()
        qcp.append(c)
    q_all[myrows, :] = q_my[x]

    def acopy(i):
        cols = pl.ds(pl.multiple_of(par * FF + i * FC, FC), FC)
        return rcopy(a_my.at[theirs, pl.ds(i * FC, FC)], a_cat.at[pl.ds(0, T), cols], as_.at[i], ar.at[i], pair)

    phase('fwait')
    fcp.wait_recv()
    def gate_up(i):
        phase(f'gu{i}')
        cols = slice(i * FC, (i + 1) * FC)
        cgu[2 * i].wait()
        g = mm(h_all[...], wg_s[:, cols])[0:T2].astype(BF16).astype(F32)
        cgu[2 * i + 1].wait()
        u = mm(h_all[...], wu_s[:, cols])[0:T2].astype(BF16).astype(F32)
        a_my[:, cols] = (g * jax.nn.sigmoid(g) * u).astype(BF16)
        acopy(i).start()
        a_cat[0:T, pl.ds(pl.multiple_of(par * FF + i * FC, FC), FC)] = a_my[mine, cols]
    gate_up(0)
    phase('k1wait')
    for d in RING:
        when(k1_in[d], lambda d=d: k1(d).wait_recv())
        for dz in RING:
            when(z_out[dz], lambda d=d, dz=dz: k2(d, dz).start())

        @pl.when(z_in[d])
        def _(d=d):
            v1(d).wait_recv()
            for dy in RING:
                v2(d, dy).start()
    gate_up(1)
    for c in co:
        c.start()

    phase('qwait')
    for c in qcp:
        c.wait_recv()
    q3 = jnp.concatenate([q_all[:, g * HEAD_DIM:(g + 1) * HEAD_DIM] for g in range(3)], axis=0)

    def scores(zz):
        kz = kv_all[0, zz].reshape(512, HEAD_DIM)
        return lax.dot_general(q3, kz, (((1,), (1,)), ((), ())), preferred_element_type=F32) * (HEAD_DIM ** -0.5)

    for d in RING:
        when(v20_in[d], lambda d=d: v2(0, d).wait_recv())
    phase('row0')
    row_tok = y * R + jnp.concatenate([lax.broadcasted_iota(jnp.int32, (R, 512), 0)] * 3, axis=0)
    col_tok = lax.broadcasted_iota(jnp.int32, (3 * R, 512), 1)
    s = jnp.where(col_tok <= row_tok, scores(z), NEG)
    m0 = jnp.max(s, axis=-1, keepdims=True)
    e = jnp.exp(s - m0)
    mx_s[...] = m0
    sum_s[...] = jnp.sum(e, axis=-1, keepdims=True)
    acc_s[...] = mm(e.astype(BF16), kv_all[1, z].reshape(512, HEAD_DIM))

    for dz in RING:
        phase(f'row{dz}')

        @pl.when(z_in[dz])
        def _(dz=dz):
            zz = z - dz
            for dy in (0,) + RING:
                k2(dy, dz).wait_recv()
            for dy in RING:
                v2(dz, dy).wait_recv()
            s = scores(zz)
            m_old = mx_s[...]
            m_new = jnp.maximum(m_old, jnp.max(s, axis=-1, keepdims=True))
            e = jnp.exp(s - m_new)
            f = jnp.exp(m_old - m_new)
            mx_s[...] = m_new
            sum_s[...] = sum_s[...] * f + jnp.sum(e, axis=-1, keepdims=True)
            acc_s[...] = acc_s[...] * f + mm(e.astype(BF16), kv_all[1, zz].reshape(512, HEAD_DIM))

    phase('osend')
    o3 = (acc_s[...] / sum_s[...]).astype(BF16)
    for g in range(3):
        o_my[:, g * HEAD_DIM:(g + 1) * HEAD_DIM] = o3[g * R:(g + 1) * R]
    ocol = pl.ds(pl.multiple_of(x * GW, GW), GW)
    ocp = []
    for d in RING:
        rows = pl.ds(pl.multiple_of(lax.rem(x + d, 4) * T, T), T)
        c = rcopy(o_my.at[rows], o_cat.at[pl.ds(0, T), ocol], os_.at[d - 1], orr.at[d - 1], xp(d))
        c.start()
        ocp.append(c)
    o_cat[0:T, ocol] = o_my[myrows, :]
    out_k[...] = kx[...].astype(BF16)
    out_v[...] = vx[...].astype(BF16)

    phase('await')
    for i in range(2):
        acopy(i).wait_recv()
    cda.wait()

    def mcopy(i):
        b = pl.ds(groups[i][1], NG)
        return rcopy(m_my.at[:, b], m_oth.at[:, b], ds_.at[i], dr.at[i], mate)

    def down(i):
        ref, at = groups[i]
        cdw[i].wait()
        m_my[:, at:at + NG] = (mm(a_cat[:, LO:], ref[...])[0:T] + mm(a_cat[:, 0:LO], wda_s[:, at:at + NG])[0:T]).astype(BF16)
        mcopy(i).start()

    def pcopy(i):
        b = pl.ds(i * 1024, 1024)
        return rcopy(p_my.at[:, b], p_oth.at[:, b], ds_.at[6 + i], dr.at[6 + i], mate)

    phase('down0')
    for i in range(3):
        down(i)
    phase('down1')
    for i in range(3, 6):
        down(i)
    phase('owait')
    for c in ocp:
        c.wait_recv()
    for i in range(3):
        phase(f'wo{i}')
        co[i].wait()
        cols = slice(i * 1024, (i + 1) * 1024)
        p_my[:, cols] = mm(o_cat[...], woref[i][...])[0:T].astype(BF16)
        pcopy(i).start()
    phase('final')

    order = (3, 4, 5, 1, 2, 0)

    def final(i):
        cols = slice(groups[i][1], groups[i][1] + NG)
        mcopy(i).wait_recv()
        out_h[:, cols] = (hid_s[:, cols].astype(F32) + (p_my[:, cols].astype(F32) + p_oth[:, cols].astype(F32))
                          + (m_my[:, cols].astype(F32) + m_oth[:, cols].astype(F32))).astype(BF16)

    for i in range(3):
        pcopy(i).wait_recv()
        final(order[2 * i])
        final(order[2 * i + 1])

    phase('drain')
    for c in [hcp, fcp] + qcp + list(kcp.values()) + ocp + [mcopy(i) for i in range(6)] + [pcopy(i) for i in range(3)]:
        c.wait_send()
    for i in range(2):
        acopy(i).wait_send()
    for d in RING:
        when(k1_out[d], lambda d=d: k1(d).wait_send())
        when(v20_out[d], lambda d=d: v2(0, d).wait_send())

        for dy in range(4):
            when(z_out[d], lambda d=d, dy=dy: k2(dy, d).wait_send())
        when(z_out[d], lambda d=d: v1(d).wait_send())

        @pl.when(z_in[d])
        def _(d=d):
            for dy in RING:
                v2(d, dy).wait_send()
    phase(None)


def emit(h, k, v, out_h, out_k, out_v, sem):
    cps = [pltpu.make_async_copy(a, b, sem.at[i]) for i, (a, b) in enumerate(((h, out_h), (k, out_k), (v, out_v)))]
    for c in cps:
        c.start()
    for c in cps:
        c.wait()


def solution(mesh):
    inv = (1.0 / (np.float32(ROPE_BASE) ** (np.arange(0, HEAD_DIM, 2, dtype=np.float32) / np.float32(HEAD_DIM)))).astype(np.float32)
    inv = np.repeat(inv, 2).reshape(1, HEAD_DIM)

    def local_layer(hidden, positions, ln_gain, w_q, w_k, w_v, w_o, w_gate, w_up, w_down):
        vm = pl.BlockSpec(memory_space=pltpu.VMEM)
        hb = pl.BlockSpec(memory_space=pl.ANY)
        dma = pltpu.SemaphoreType.DMA
        V = pltpu.VMEM
        scratch = [
            V((T, D), BF16), V((1, T), jnp.int32), V((D // HEAD_DIM, HEAD_DIM), BF16), V((1, HEAD_DIM), F32),
            V((D, QW), BF16), V((D, KW), BF16), V((D, KW), BF16),
            V((D, FF), BF16), V((D, FF), BF16), V((LO, D), BF16), V((D, KW), BF16),
            V((R, D), BF16), V((T, QW), F32), V((T, KW), F32), V((T, KW), F32), V((R, HEAD_DIM), F32), V((R, HEAD_DIM), F32),
            V((4, T, GW), BF16), V((R, GW), BF16), V((4, 2, T, HEAD_DIM), BF16), V((2, 4, 4, R, HEAD_DIM), BF16),
            V((3 * R, 1), F32), V((3 * R, 1), F32), V((3 * R, HEAD_DIM), F32), V((R, GW), BF16), V((R, QW), BF16),
            V((T2, FF), BF16), V((R, FFT), BF16), V((T, D), BF16), V((T, D), BF16), V((T, D), BF16), V((T, D), BF16),
            dma((4,)), dma((26,)), dma((3,)), dma((3,)), dma((3,)), dma((3,)), dma((3,)), dma((3,)), dma((3,)), dma((3,)),
            dma((3,)), dma((3,)), dma((3,)), dma((3,)), dma((12,)), dma((12,)), dma((12,)), dma((12,)),
            dma((6,)), dma((6,)), dma((3,)), dma((3,)), dma((9,)), dma((9,)),
        ]
        outs = (jax.ShapeDtypeStruct((T, D), BF16), jax.ShapeDtypeStruct((R, HEAD_DIM), BF16), jax.ShapeDtypeStruct((R, HEAD_DIM), BF16))
        res = pl.pallas_call(
            kernel,
            name='layer',
            out_shape=tuple(pltpu.VMEM(o.shape, o.dtype) for o in outs),
            in_specs=[hb] * 11,
            out_specs=(vm, vm, vm),
            scratch_shapes=scratch,
            compiler_params=pltpu.CompilerParams(collective_id=0, has_side_effects=True, vmem_limit_bytes=60000000),
        )(hidden, positions.reshape(1, T), ln_gain.reshape(D // HEAD_DIM, HEAD_DIM), jnp.asarray(inv),
          w_q, w_k, w_v, w_o, w_gate, w_up, w_down)
        out_h, out_k, out_v = pl.pallas_call(
            emit,
            name='emit',
            out_shape=outs,
            in_specs=[vm] * 3,
            out_specs=(hb, hb, hb),
            scratch_shapes=[dma((3,))],
        )(*[pltpu.with_memory_space_constraint(r, pltpu.VMEM) for r in res])
        return out_h, out_k.reshape(T, 4, HEAD_DIM), out_v.reshape(T, 4, HEAD_DIM)

    row_spec = P(('dp', 'cp'), None)
    col_spec = P(None, 'tp')
    cache_spec = P(('dp', 'cp'), 'tp', None)
    in_specs = (row_spec, P(('dp', 'cp')), P(None), col_spec, col_spec, col_spec, P('tp', None), col_spec, col_spec, P('tp', None))
    return jax.shard_map(local_layer, mesh=mesh, in_specs=in_specs, out_specs=(row_spec, cache_spec, cache_spec), check_vma=False)
```

```python
import jax
import jax.numpy as jnp
import numpy as np
from jax import lax
from jax.experimental import pallas as pl
from jax.experimental.pallas import tpu as pltpu
from jax.sharding import PartitionSpec as P

HEAD_DIM = 128
ROPE_BASE = 4000000
LN_EPS = 1e-5
D = 3072
T = 32
R = 128
QW = 1536
KW = 512
GW = 384
T2 = 64
FF = 2048
FC = 1024
LO = 1024
FFT = 4096
KC = 4
NG = 512
NEG = -1e30
SCALE = HEAD_DIM ** -0.5 * 1.4426950408889634
F32 = jnp.float32
BF16 = jnp.bfloat16
RING = (1, 3, 2)


def mm(a, b):
    return jnp.dot(a, b, preferred_element_type=F32)


def rope(x, cos, sin, even):
    left = pltpu.roll(x, 127, 1)
    right = pltpu.roll(x, 1, 1)
    return (x * cos + jnp.where(even, -left, right) * sin).astype(BF16)


def kernel(hid, pos, gain, invf, wq, wk, wv, wo, wg, wu, wd,
           out_h, out_k, out_v,
           hid_s, pos_s, gain_s, inv_s,
           wq_s, wk_s, wv_s, wg_s, wu_s, wda_s, wdx_s,
           h_all, accq, acck, accv, kx, vx, q_my, q_all, kv_my, kv_all,
           mx_s, sum_s, acc_s, o_my, o_cat,
           a_my, a_cat, p_acc, m_my, m_oth, p_my, p_oth,
           i_sem, w_sem, hs, hr, fs, fr, qs, qr, ks, kr, k1s, k1r, v1s, v1r, k2s, k2r, v2s, v2r,
           as_, ar, os_, orr, ds_, dr):
    scope = []

    def phase(name):
        if scope:
            scope.pop().__exit__(None, None, None)
        if name:
            scope.append(jax.named_scope(name))
            scope[0].__enter__()

    phase('start')
    tp = lax.axis_index('tp')
    cp = lax.axis_index('cp')
    x = lax.rem(cp, 4)
    y = lax.rem(cp // 4, 4)
    z = cp // 16

    def xp(d):
        return tp, z * 16 + y * 4 + lax.rem(x + d, 4)

    def yp(d):
        return tp, z * 16 + lax.rem(y + d, 4) * 4 + x

    def zp(d):
        return tp, lax.rem(z + d, 4) * 16 + y * 4 + x

    mate = (1 - tp, cp)

    def rcopy(src, dst, ss, rs, dev):
        return pltpu.make_async_remote_copy(
            src_ref=src, dst_ref=dst, send_sem=ss, recv_sem=rs,
            device_id={'tp': dev[0], 'cp': dev[1]}, device_id_type=pl.DeviceIdType.MESH)

    small = [pltpu.make_async_copy(a, b, i_sem.at[i])
             for i, (a, b) in enumerate(((hid, hid_s), (gain, gain_s), (pos, pos_s), (invf, inv_s)))]
    for c in small:
        c.start()
    half = D // 2
    ckv = [pltpu.make_async_copy(src.at[pl.ds(i * half, half)], dst.at[pl.ds(i * half, half)], w_sem.at[2 * i + n])
           for i in range(2) for n, (src, dst) in enumerate(((wk, wk_s), (wv, wv_s)))]
    kc = D // KC
    cwq = [pltpu.make_async_copy(wq.at[pl.ds(i * kc, kc)], wq_s.at[pl.ds(i * kc, kc)], w_sem.at[4 + i]) for i in range(KC)]
    par = lax.rem(x, 2)
    pair = (tp, cp + 1 - 2 * par)
    mine = pl.ds(pl.multiple_of(par * T, T), T)
    theirs = pl.ds(pl.multiple_of((1 - par) * T, T), T)
    hcol = pl.ds(pl.multiple_of(tp * QW, QW), QW)
    cgu = [pltpu.make_async_copy(src.at[:, pl.ds(pl.multiple_of(par * FF + i * FC, FC), FC)],
                                 dst.at[:, pl.ds(i * FC, FC)], w_sem.at[8 + 2 * i + n])
           for i in range(2) for n, (src, dst) in enumerate(((wg, wg_s), (wu, wu_s)))]
    cda = pltpu.make_async_copy(wd.at[pl.ds(0, LO)], wda_s, w_sem.at[16])
    woref = [wg_s.at[pl.ds(0, QW), pl.ds(0, 1024)], wg_s.at[pl.ds(0, QW), pl.ds(1024, 1024)], wg_s.at[pl.ds(QW, QW), pl.ds(0, 1024)]]
    co = [pltpu.make_async_copy(wo.at[:, pl.ds(i * 1024, 1024)], woref[i], w_sem.at[17 + i]) for i in range(3)]
    groups = [(wdx_s.at[:], 5 * NG), (wk_s.at[:], 3 * NG), (wv_s.at[:], 4 * NG)] + [
        (wq_s.at[:, pl.ds(i * NG, NG)], i * NG) for i in range(3)]
    low = pl.ds(LO, D)
    cdw = [pltpu.make_async_copy(wd.at[low, pl.ds(at, NG)], ref, w_sem.at[20 + i]) for i, (ref, at) in enumerate(groups)]
    for c in ckv:
        c.start(priority=1)

    barrier = pltpu.get_barrier_semaphore()
    peers = [f(d) for f in (xp, yp, zp) for d in (1, 2, 3)] + [mate]
    for dev in peers:
        pl.semaphore_signal(barrier, inc=1, device_id={'tp': dev[0], 'cp': dev[1]}, device_id_type=pl.DeviceIdType.MESH)

    h_all[T2:R, :] = jnp.zeros((R - T2, D), BF16)
    a_cat[T:R, :] = jnp.zeros((R - T, FFT), BF16)
    o_cat[T:R, :] = jnp.zeros((R - T, QW), BF16)

    for yy in range(4):
        @pl.when(yy > y)
        def _(yy=yy):
            kv_all[1, z, yy] = jnp.zeros((R, HEAD_DIM), BF16)

        @pl.when(jnp.logical_and(yy > y, z == 3))
        def _(yy=yy):
            kv_all[0, z, yy] = jnp.zeros((R, HEAD_DIM), BF16)

    phase('ln')
    for c in small:
        c.wait()
    for c in cwq + cgu + [cda, cdw[0]]:
        c.start(priority=1)
    hf = hid_s[...].astype(F32)
    mean = jnp.sum(hf, axis=-1, keepdims=True) * (1.0 / D)
    cen = hf - mean
    var = jnp.sum(cen * cen, axis=-1, keepdims=True) * (1.0 / D)
    scaled = cen * lax.rsqrt(var + LN_EPS)
    gf = gain_s[...].astype(F32)
    myrows = pl.ds(pl.multiple_of(x * T, T), T)
    for i in range(D // HEAD_DIM):
        cols = slice(i * HEAD_DIM, (i + 1) * HEAD_DIM)
        h_all[mine, cols] = (scaled[:, cols] * gf[i:i + 1]).astype(BF16)

    hcp = rcopy(h_all.at[mine, hcol], h_all.at[mine, hcol], hs.at[0], hr.at[0], pair)
    fcp = rcopy(h_all.at[theirs, hcol], h_all.at[theirs, hcol], fs.at[0], fr.at[0], mate)
    kcp = {d: rcopy(kv_my.at[lax.rem(x + d, 4)], kv_all.at[:, z, y, myrows], ks.at[d - 1], kr.at[d - 1], xp(d)) for d in RING}

    phase('tables')
    diag = lax.broadcasted_iota(jnp.int32, (T, T), 0) == lax.broadcasted_iota(jnp.int32, (T, T), 1)
    posf = jnp.sum(jnp.where(diag, jnp.broadcast_to(pos_s[...].astype(F32), (T, T)), 0.0), axis=1, keepdims=True)
    ang = posf * inv_s[...]
    cos = jnp.cos(ang)
    sin = jnp.sin(ang)
    even = lax.rem(lax.broadcasted_iota(jnp.int32, (T, HEAD_DIM), 1), 2) == 0

    phase('kvproj')
    for i in range(2):
        rows = slice(i * half, (i + 1) * half)
        for n, (w, acc) in enumerate(((wk_s, acck), (wv_s, accv))):
            ckv[2 * i + n].wait()
            part = mm(h_all[mine, rows], w[rows, :])
            if i == 0:
                acc[...] = part
            else:
                acc[...] += part
    phase('kvrope')
    for j in range(4):
        cols = slice(j * HEAD_DIM, (j + 1) * HEAD_DIM)
        kj = rope(acck[:, cols].astype(BF16).astype(F32), cos, sin, even)
        vj = accv[:, cols].astype(BF16)
        kv_my[j, 0] = kj
        kv_my[j, 1] = vj
        kx[pl.ds(j, T, stride=4), :] = kj.astype(F32)
        vx[pl.ds(j, T, stride=4), :] = vj.astype(F32)
    kv_all[:, z, y, myrows, :] = kv_my[x]

    phase('barrier')
    pl.semaphore_wait(barrier, len(peers))
    for d in RING:
        kcp[d].start()
    hcp.start()

    phase('qproj')
    for i in range(KC):
        rows = slice(i * kc, (i + 1) * kc)
        cwq[i].wait()
        part = mm(h_all[mine, rows], wq_s[rows, :])
        if i == 0:
            accq[...] = part
        else:
            accq[...] += part
    for c in cdw[1:]:
        c.start(priority=1)

    def k1(d):
        b = kv_all.at[0, z, y]
        return rcopy(b, b, k1s.at[d - 1], k1r.at[d - 1], yp(d))

    def v1(d):
        b = kv_all.at[1, z, y]
        return rcopy(b, b, v1s.at[d - 1], v1r.at[d - 1], zp(d))

    def k2(dy, dz):
        b = kv_all.at[0, z, lax.rem(y + 4 - dy, 4)]
        return rcopy(b, b, k2s.at[3 * dy + dz - 1], k2r.at[3 * dy + dz - 1], zp(dz))

    def v2(dz, dy):
        b = kv_all.at[1, lax.rem(z + 4 - dz, 4), y]
        return rcopy(b, b, v2s.at[3 * dz + dy - 1], v2r.at[3 * dz + dy - 1], yp(dy))

    k1_out = {d: jnp.logical_or(y + d <= 3, z < 3) for d in RING}
    k1_in = {d: jnp.logical_or(y >= d, z < 3) for d in RING}
    z_out = {d: z + d <= 3 for d in RING}
    z_in = {d: z >= d for d in RING}
    v20_out = {d: y + d <= 3 for d in RING}
    v20_in = {d: y >= d for d in RING}

    def when(cond, fn):
        pl.when(cond)(lambda: fn())

    phase('kvx')
    for d in RING:
        kcp[d].wait_recv()
    for d in RING:
        when(k1_out[d], lambda d=d: k1(d).start())
        when(z_out[d], lambda d=d: v1(d).start())
    for d in RING:
        when(z_out[d], lambda d=d: k2(0, d).start())
    for d in RING:
        when(v20_out[d], lambda d=d: v2(0, d).start())

    phase('hwait')
    hcp.wait_recv()
    fcp.start()

    phase('qrope')
    for j in range(12):
        cols = slice(j * HEAD_DIM, (j + 1) * HEAD_DIM)
        q_my[j // 3, :, (j % 3) * HEAD_DIM:(j % 3 + 1) * HEAD_DIM] = rope(
            accq[:, cols].astype(BF16).astype(F32), cos, sin, even)
    qcp = []
    for d in RING:
        dst = lax.rem(x + d, 4)
        c = rcopy(q_my.at[dst], q_all.at[myrows], qs.at[d - 1], qr.at[d - 1], xp(d))
        c.start()
        qcp.append(c)
    q_all[myrows, :] = q_my[x]

    def acopy(i):
        cols = pl.ds(pl.multiple_of(par * FF + i * FC, FC), FC)
        return rcopy(a_my.at[theirs, pl.ds(i * FC, FC)], a_cat.at[pl.ds(0, T), cols], as_.at[i], ar.at[i], pair)

    phase('fwait')
    fcp.wait_recv()
    def gate_up(i):
        phase(f'gu{i}')
        cols = slice(i * FC, (i + 1) * FC)
        cgu[2 * i].wait()
        g = mm(h_all[...], wg_s[:, cols])[0:T2].astype(BF16).astype(F32)
        cgu[2 * i + 1].wait()
        u = mm(h_all[...], wu_s[:, cols])[0:T2].astype(BF16).astype(F32)
        a_my[:, cols] = (g * jax.nn.sigmoid(g) * u).astype(BF16)
        acopy(i).start()
        a_cat[0:T, pl.ds(pl.multiple_of(par * FF + i * FC, FC), FC)] = a_my[mine, cols]
    gate_up(0)
    phase('k1wait')
    for d in RING:
        when(k1_in[d], lambda d=d: k1(d).wait_recv())
        for dz in RING:
            when(z_out[dz], lambda d=d, dz=dz: k2(d, dz).start())

        @pl.when(z_in[d])
        def _(d=d):
            v1(d).wait_recv()
            for dy in RING:
                v2(d, dy).start()
    gate_up(1)
    for c in co:
        c.start(priority=1)

    phase('qwait')
    for c in qcp:
        c.wait_recv()
    q3 = jnp.concatenate([q_all[:, g * HEAD_DIM:(g + 1) * HEAD_DIM] for g in range(3)], axis=0)

    def scores(zz):
        kz = kv_all[0, zz].reshape(512, HEAD_DIM)
        return lax.dot_general(q3, kz, (((1,), (1,)), ((), ())), preferred_element_type=F32)

    for d in RING:
        when(v20_in[d], lambda d=d: v2(0, d).wait_recv())
    phase('row0')
    row_tok = y * R + jnp.concatenate([lax.broadcasted_iota(jnp.int32, (R, 512), 0)] * 3, axis=0)
    col_tok = lax.broadcasted_iota(jnp.int32, (3 * R, 512), 1)
    s = jnp.where(col_tok <= row_tok, scores(z), NEG)
    m0 = jnp.max(s, axis=-1, keepdims=True)
    e = jnp.exp2((s - m0) * SCALE)
    mx_s[...] = m0
    sum_s[...] = jnp.sum(e, axis=-1, keepdims=True)
    acc_s[...] = mm(e.astype(BF16), kv_all[1, z].reshape(512, HEAD_DIM))

    def mcopy(i):
        b = pl.ds(groups[i][1], NG)
        return rcopy(m_my.at[:, b], m_oth.at[:, b], ds_.at[i], dr.at[i], mate)

    def down(i):
        ref, at = groups[i]
        cdw[i].wait()
        m_my[:, at:at + NG] = (mm(a_cat[:, LO:], ref[...])[0:T] + mm(a_cat[:, 0:LO], wda_s[:, at:at + NG])[0:T]).astype(BF16)
        mcopy(i).start()

    def pcopy(i):
        b = pl.ds(i * 1024, 1024)
        return rcopy(p_my.at[:, b], p_oth.at[:, b], ds_.at[6 + i], dr.at[6 + i], mate)

    def first_down():
        for i in range(2):
            acopy(i).wait_recv()
        cda.wait()
        for i in range(2):
            down(i)

    late = jnp.logical_and(jnp.logical_and(z == 3, y <= 1), x < 2)
    phase('downB')
    pl.when(late)(first_down)

    for dz in RING:
        phase(f'row{dz}')

        @pl.when(z_in[dz])
        def _(dz=dz):
            zz = z - dz
            for dy in (0,) + RING:
                k2(dy, dz).wait_recv()
            for dy in RING:
                v2(dz, dy).wait_recv()
            s = scores(zz)
            m_old = mx_s[...]
            m_new = jnp.maximum(m_old, jnp.max(s, axis=-1, keepdims=True))
            e = jnp.exp2((s - m_new) * SCALE)
            f = jnp.exp2((m_old - m_new) * SCALE)
            mx_s[...] = m_new
            sum_s[...] = sum_s[...] * f + jnp.sum(e, axis=-1, keepdims=True)
            acc_s[...] = acc_s[...] * f + mm(e.astype(BF16), kv_all[1, zz].reshape(512, HEAD_DIM))

    phase('osend')
    o3 = (acc_s[...] / sum_s[...]).astype(BF16)
    for g in range(3):
        o_my[:, g * HEAD_DIM:(g + 1) * HEAD_DIM] = o3[g * R:(g + 1) * R]
    ocol = pl.ds(pl.multiple_of(x * GW, GW), GW)
    ocp = []
    for d in RING:
        rows = pl.ds(pl.multiple_of(lax.rem(x + d, 4) * T, T), T)
        c = rcopy(o_my.at[rows], o_cat.at[pl.ds(0, T), ocol], os_.at[d - 1], orr.at[d - 1], xp(d))
        c.start()
        ocp.append(c)
    o_cat[0:T, ocol] = o_my[myrows, :]
    out_k[...] = kx[...].astype(BF16)
    out_v[...] = vx[...].astype(BF16)

    phase('down0')
    pl.when(jnp.logical_not(late))(first_down)
    down(2)
    phase('down1')
    for i in range(3, 6):
        down(i)
    def wo_part(frm, first, last):
        src = lax.rem(frm, 4)
        cols = pl.ds(pl.multiple_of(src * GW, GW), GW)
        rows = pl.ds(pl.multiple_of(src * GW, GW), GW)
        for i in range(3):
            pcols = slice(i * 1024, (i + 1) * 1024)
            part = mm(o_cat[:, cols], woref[i][rows, :])[0:T]
            if not first:
                part = p_acc[:, pcols] + part
            if last:
                p_my[:, pcols] = part.astype(BF16)
                pcopy(i).start()
            else:
                p_acc[:, pcols] = part

    phase('woown')
    for c in co:
        c.wait()
    wo_part(x, True, False)
    for n, d in enumerate(RING):
        phase(f'owait{d}')
        ocp[n].wait_recv()
        phase(f'wo{d}')
        wo_part(x + 4 - d, False, n == 2)
    phase('final')

    order = (3, 4, 5, 1, 2, 0)

    def final(i):
        cols = slice(groups[i][1], groups[i][1] + NG)
        mcopy(i).wait_recv()
        out_h[:, cols] = (hid_s[:, cols].astype(F32) + (p_my[:, cols].astype(F32) + p_oth[:, cols].astype(F32))
                          + (m_my[:, cols].astype(F32) + m_oth[:, cols].astype(F32))).astype(BF16)

    for i in range(3):
        pcopy(i).wait_recv()
        final(order[2 * i])
        final(order[2 * i + 1])

    phase('drain')
    for c in [hcp, fcp] + qcp + list(kcp.values()) + ocp + [mcopy(i) for i in range(6)] + [pcopy(i) for i in range(3)]:
        c.wait_send()
    for i in range(2):
        acopy(i).wait_send()
    for d in RING:
        when(k1_out[d], lambda d=d: k1(d).wait_send())
        when(v20_out[d], lambda d=d: v2(0, d).wait_send())

        for dy in range(4):
            when(z_out[d], lambda d=d, dy=dy: k2(dy, d).wait_send())
        when(z_out[d], lambda d=d: v1(d).wait_send())

        @pl.when(z_in[d])
        def _(d=d):
            for dy in RING:
                v2(d, dy).wait_send()
    phase(None)


def emit(h, k, v, out_h, out_k, out_v, sem):
    cps = [pltpu.make_async_copy(a, b, sem.at[i]) for i, (a, b) in enumerate(((h, out_h), (k, out_k), (v, out_v)))]
    for c in cps:
        c.start()
    for c in cps:
        c.wait()


def solution(mesh):
    inv = (1.0 / (np.float32(ROPE_BASE) ** (np.arange(0, HEAD_DIM, 2, dtype=np.float32) / np.float32(HEAD_DIM)))).astype(np.float32)
    inv = np.repeat(inv, 2).reshape(1, HEAD_DIM)

    def local_layer(hidden, positions, ln_gain, w_q, w_k, w_v, w_o, w_gate, w_up, w_down):
        vm = pl.BlockSpec(memory_space=pltpu.VMEM)
        hb = pl.BlockSpec(memory_space=pl.ANY)
        dma = pltpu.SemaphoreType.DMA
        V = pltpu.VMEM
        scratch = [
            V((T, D), BF16), V((1, T), jnp.int32), V((D // HEAD_DIM, HEAD_DIM), BF16), V((1, HEAD_DIM), F32),
            V((D, QW), BF16), V((D, KW), BF16), V((D, KW), BF16),
            V((D, FF), BF16), V((D, FF), BF16), V((LO, D), BF16), V((D, KW), BF16),
            V((R, D), BF16), V((T, QW), F32), V((T, KW), F32), V((T, KW), F32), V((R, HEAD_DIM), F32), V((R, HEAD_DIM), F32),
            V((4, T, GW), BF16), V((R, GW), BF16), V((4, 2, T, HEAD_DIM), BF16), V((2, 4, 4, R, HEAD_DIM), BF16),
            V((3 * R, 1), F32), V((3 * R, 1), F32), V((3 * R, HEAD_DIM), F32), V((R, GW), BF16), V((R, QW), BF16),
            V((T2, FF), BF16), V((R, FFT), BF16), V((T, D), F32), V((T, D), BF16), V((T, D), BF16), V((T, D), BF16), V((T, D), BF16),
            dma((4,)), dma((26,)), dma((3,)), dma((3,)), dma((3,)), dma((3,)), dma((3,)), dma((3,)), dma((3,)), dma((3,)),
            dma((3,)), dma((3,)), dma((3,)), dma((3,)), dma((12,)), dma((12,)), dma((12,)), dma((12,)),
            dma((6,)), dma((6,)), dma((3,)), dma((3,)), dma((9,)), dma((9,)),
        ]
        outs = (jax.ShapeDtypeStruct((T, D), BF16), jax.ShapeDtypeStruct((R, HEAD_DIM), BF16), jax.ShapeDtypeStruct((R, HEAD_DIM), BF16))
        res = pl.pallas_call(
            kernel,
            name='layer',
            out_shape=tuple(pltpu.VMEM(o.shape, o.dtype) for o in outs),
            in_specs=[hb] * 11,
            out_specs=(vm, vm, vm),
            scratch_shapes=scratch,
            compiler_params=pltpu.CompilerParams(collective_id=0, has_side_effects=True, vmem_limit_bytes=60000000),
        )(hidden, positions.reshape(1, T), ln_gain.reshape(D // HEAD_DIM, HEAD_DIM), jnp.asarray(inv),
          w_q, w_k, w_v, w_o, w_gate, w_up, w_down)
        out_h, out_k, out_v = pl.pallas_call(
            emit,
            name='emit',
            out_shape=outs,
            in_specs=[vm] * 3,
            out_specs=(hb, hb, hb),
            scratch_shapes=[dma((3,))],
        )(*[pltpu.with_memory_space_constraint(r, pltpu.VMEM) for r in res])
        return out_h, out_k.reshape(T, 4, HEAD_DIM), out_v.reshape(T, 4, HEAD_DIM)

    row_spec = P(('dp', 'cp'), None)
    col_spec = P(None, 'tp')
    cache_spec = P(('dp', 'cp'), 'tp', None)
    in_specs = (row_spec, P(('dp', 'cp')), P(None), col_spec, col_spec, col_spec, P('tp', None), col_spec, col_spec, P('tp', None))
    return jax.shard_map(local_layer, mesh=mesh, in_specs=in_specs, out_specs=(row_spec, cache_spec, cache_spec), check_vma=False)
```

```python
import jax
import jax.numpy as jnp
import numpy as np
from jax import lax
from jax.experimental import pallas as pl
from jax.experimental.pallas import tpu as pltpu
from jax.sharding import PartitionSpec as P

HEAD_DIM = 128
ROPE_BASE = 4000000
LN_EPS = 1e-5
D = 3072
T = 32
R = 128
QW = 1536
KW = 512
GW = 384
T2 = 64
FF = 2048
FC = 1024
LO = 1024
FFT = 4096
KC = 2
Q2 = 768
NG = 512
NEG = -1e30
SCALE = HEAD_DIM ** -0.5 * 1.4426950408889634
F32 = jnp.float32
BF16 = jnp.bfloat16
RING = (1, 3, 2)


def mm(a, b):
    return jnp.dot(a, b, preferred_element_type=F32)


def rope(x, cos, sin, even):
    left = pltpu.roll(x, 127, 1)
    right = pltpu.roll(x, 1, 1)
    return (x * cos + jnp.where(even, -left, right) * sin).astype(BF16)


def kernel(hid, pos, gain, invf, wq, wk, wv, wo, wg, wu, wd,
           out_h, out_k, out_v,
           hid_s, pos_s, gain_s, inv_s,
           wq_s, wk_s, wv_s, wg_s, wu_s, wda_s, wdx_s,
           h_all, cs_s, accq, acck, accv, kx, vx, q_my, q_all, kv_my, kv_all,
           mx_s, sum_s, acc_s, o_my, o_cat,
           a_my, a_cat, m_my, m_oth, p_my, p_oth,
           i_sem, w_sem, cs_sem, hs, hr, fs, fr, qs, qr, ks, kr, k1s, k1r, v1s, v1r, k2s, k2r, v2s, v2r,
           as_, ar, os_, orr, ds_, dr):
    scope = []

    def phase(name):
        if scope:
            scope.pop().__exit__(None, None, None)
        if name:
            scope.append(jax.named_scope(name))
            scope[0].__enter__()

    phase('start')
    tp = lax.axis_index('tp')
    cp = lax.axis_index('cp')
    x = lax.rem(cp, 4)
    y = lax.rem(cp // 4, 4)
    z = cp // 16

    def xp(d):
        return tp, z * 16 + y * 4 + lax.rem(x + d, 4)

    def yp(d):
        return tp, z * 16 + lax.rem(y + d, 4) * 4 + x

    def zp(d):
        return tp, lax.rem(z + d, 4) * 16 + y * 4 + x

    mate = (1 - tp, cp)

    def when(cond, fn):
        pl.when(cond)(lambda: fn())

    def rcopy(src, dst, ss, rs, dev):
        return pltpu.make_async_remote_copy(
            src_ref=src, dst_ref=dst, send_sem=ss, recv_sem=rs,
            device_id={'tp': dev[0], 'cp': dev[1]}, device_id_type=pl.DeviceIdType.MESH)

    small = [pltpu.make_async_copy(a, b, i_sem.at[i])
             for i, (a, b) in enumerate(((hid, hid_s), (gain, gain_s), (pos, pos_s), (invf, inv_s)))]
    for c in small:
        c.start()
    half = D // 2
    ckv = [pltpu.make_async_copy(src.at[pl.ds(i * half, half)], dst.at[pl.ds(i * half, half)], w_sem.at[2 * i + n])
           for i in range(2) for n, (src, dst) in enumerate(((wk, wk_s), (wv, wv_s)))]
    kc = D // KC
    par = lax.rem(x, 2)
    pair = (tp, cp + 1 - 2 * par)
    qcol = pl.ds(pl.multiple_of(par * Q2, Q2), Q2)
    cwq = [pltpu.make_async_copy(wq.at[pl.ds(i * kc, kc), qcol], wq_s.at[pl.ds(i * kc, kc), pl.ds(0, Q2)], w_sem.at[4 + i]) for i in range(KC)]
    mine = pl.ds(pl.multiple_of(par * T, T), T)
    theirs = pl.ds(pl.multiple_of((1 - par) * T, T), T)
    hcol = pl.ds(pl.multiple_of(tp * QW, QW), QW)
    cgu = [pltpu.make_async_copy(src.at[:, pl.ds(pl.multiple_of(par * FF + i * FC, FC), FC)],
                                 dst.at[:, pl.ds(i * FC, FC)], w_sem.at[8 + 2 * i + n])
           for i in range(2) for n, (src, dst) in enumerate(((wg, wg_s), (wu, wu_s)))]
    cda = pltpu.make_async_copy(wd.at[pl.ds(0, LO)], wda_s, w_sem.at[16])
    woref = [wg_s.at[pl.ds(0, QW), pl.ds(0, 1024)], wg_s.at[pl.ds(0, QW), pl.ds(1024, 1024)], wg_s.at[pl.ds(QW, QW), pl.ds(0, 1024)]]
    co = [pltpu.make_async_copy(wo.at[:, pl.ds(i * 1024, 1024)], woref[i], w_sem.at[17 + i]) for i in range(3)]
    groups = [(wdx_s.at[:], 5 * NG), (wk_s.at[:], 3 * NG), (wv_s.at[:], 4 * NG)] + [
        (wq_s.at[:, pl.ds(i * NG, NG)], i * NG) for i in range(3)]
    low = pl.ds(LO, D)
    cdw = [pltpu.make_async_copy(wd.at[low, pl.ds(at, NG)], ref, w_sem.at[20 + i]) for i, (ref, at) in enumerate(groups)]
    for c in ckv:
        c.start(priority=1)

    barrier = pltpu.get_barrier_semaphore()
    peers = [f(d) for f in (xp, yp, zp) for d in (1, 2, 3)] + [mate]
    for dev in peers:
        pl.semaphore_signal(barrier, inc=1, device_id={'tp': dev[0], 'cp': dev[1]}, device_id_type=pl.DeviceIdType.MESH)

    h_all[T2:R, :] = jnp.zeros((R - T2, D), BF16)
    a_cat[T:R, :] = jnp.zeros((R - T, FFT), BF16)
    o_cat[T:R, :] = jnp.zeros((R - T, QW), BF16)

    for yy in range(4):
        @pl.when(yy > y)
        def _(yy=yy):
            kv_all[1, z, yy] = jnp.zeros((R, HEAD_DIM), BF16)

        @pl.when(jnp.logical_and(yy > y, z == 3))
        def _(yy=yy):
            kv_all[0, z, yy] = jnp.zeros((R, HEAD_DIM), BF16)

    phase('ln')
    for c in small:
        c.wait()
    for c in cwq + cgu + [cda, cdw[0]]:
        c.start(priority=1)
    hf = hid_s[...].astype(F32)
    mean = jnp.sum(hf, axis=-1, keepdims=True) * (1.0 / D)
    cen = hf - mean
    var = jnp.sum(cen * cen, axis=-1, keepdims=True) * (1.0 / D)
    scaled = cen * lax.rsqrt(var + LN_EPS)
    gf = gain_s[...].astype(F32)
    myrows = pl.ds(pl.multiple_of(x * T, T), T)
    for i in range(D // HEAD_DIM):
        cols = slice(i * HEAD_DIM, (i + 1) * HEAD_DIM)
        h_all[mine, cols] = (scaled[:, cols] * gf[i:i + 1]).astype(BF16)

    hcp = rcopy(h_all.at[mine, hcol], h_all.at[mine, hcol], hs.at[0], hr.at[0], pair)
    fcp = rcopy(h_all.at[theirs, hcol], h_all.at[theirs, hcol], fs.at[0], fr.at[0], mate)
    kcp = {d: rcopy(kv_my.at[lax.rem(x + d, 4)], kv_all.at[:, z, y, myrows], ks.at[d - 1], kr.at[d - 1], xp(d)) for d in RING}

    phase('tables')
    diag = lax.broadcasted_iota(jnp.int32, (T, T), 0) == lax.broadcasted_iota(jnp.int32, (T, T), 1)
    posf = jnp.sum(jnp.where(diag, jnp.broadcast_to(pos_s[...].astype(F32), (T, T)), 0.0), axis=1, keepdims=True)
    ang = posf * inv_s[...]
    cos = jnp.cos(ang)
    sin = jnp.sin(ang)
    even = lax.rem(lax.broadcasted_iota(jnp.int32, (T, HEAD_DIM), 1), 2) == 0
    cs_s[0, mine] = cos
    cs_s[1, mine] = sin
    cscp = rcopy(cs_s.at[:, mine], cs_s.at[:, mine], cs_sem.at[0], cs_sem.at[1], pair)

    phase('kvproj')
    for i in range(2):
        rows = slice(i * half, (i + 1) * half)
        for n, (w, acc) in enumerate(((wk_s, acck), (wv_s, accv))):
            ckv[2 * i + n].wait()
            part = mm(h_all[mine, rows], w[rows, :])
            if i == 0:
                acc[...] = part
            else:
                acc[...] += part
    phase('kvrope')
    for j in range(4):
        cols = slice(j * HEAD_DIM, (j + 1) * HEAD_DIM)
        kj = rope(acck[:, cols].astype(BF16).astype(F32), cos, sin, even)
        vj = accv[:, cols].astype(BF16)
        kv_my[j, 0] = kj
        kv_my[j, 1] = vj
        kx[pl.ds(j, T, stride=4), :] = kj.astype(F32)
        vx[pl.ds(j, T, stride=4), :] = vj.astype(F32)
    kv_all[:, z, y, myrows, :] = kv_my[x]

    phase('barrier')
    pl.semaphore_wait(barrier, len(peers))
    for d in RING:
        kcp[d].start()
    hcp.start()
    cscp.start()

    for c in cdw[1:3]:
        c.start(priority=1)

    def k1(d):
        b = kv_all.at[0, z, y]
        return rcopy(b, b, k1s.at[d - 1], k1r.at[d - 1], yp(d))

    def v1(d):
        b = kv_all.at[1, z, y]
        return rcopy(b, b, v1s.at[d - 1], v1r.at[d - 1], zp(d))

    def k2(dy, dz):
        b = kv_all.at[0, z, lax.rem(y + 4 - dy, 4)]
        return rcopy(b, b, k2s.at[3 * dy + dz - 1], k2r.at[3 * dy + dz - 1], zp(dz))

    def v2(dz, dy):
        b = kv_all.at[1, lax.rem(z + 4 - dz, 4), y]
        return rcopy(b, b, v2s.at[3 * dz + dy - 1], v2r.at[3 * dz + dy - 1], yp(dy))

    k1_out = {d: jnp.logical_or(y + d <= 3, z < 3) for d in RING}
    k1_in = {d: jnp.logical_or(y >= d, z < 3) for d in RING}
    z_out = {d: z + d <= 3 for d in RING}
    z_in = {d: z >= d for d in RING}
    v20_out = {d: y + d <= 3 for d in RING}
    v20_in = {d: y >= d for d in RING}

    phase('kvx')
    for d in RING:
        kcp[d].wait_recv()
    for d in RING:
        when(k1_out[d], lambda d=d: k1(d).start())
        when(z_out[d], lambda d=d: v1(d).start())
    for d in RING:
        when(z_out[d], lambda d=d: k2(0, d).start())
    for d in RING:
        when(v20_out[d], lambda d=d: v2(0, d).start())

    phase('hwait')
    hcp.wait_recv()
    fcp.start()

    def acopy(i):
        cols = pl.ds(pl.multiple_of(par * FF + i * FC, FC), FC)
        return rcopy(a_my.at[theirs, pl.ds(i * FC, FC)], a_cat.at[pl.ds(0, T), cols], as_.at[i], ar.at[i], pair)

    def pass_on():
        for d in RING:
            when(k1_in[d], lambda d=d: k1(d).wait_recv())
            for dz in RING:
                when(z_out[dz], lambda d=d, dz=dz: k2(d, dz).start())

            @pl.when(z_in[d])
            def _(d=d):
                v1(d).wait_recv()
                for dy in RING:
                    v2(d, dy).start()

    soon = jnp.logical_and(tp == 1, y >= 1)
    next_ = jnp.logical_and(tp == 0, y >= 2)
    last = jnp.logical_and(tp == 0, jnp.logical_and(y == 0, z < 3))
    third = jnp.logical_not(jnp.logical_or(last, jnp.logical_or(soon, next_)))

    phase('k1a')
    pl.when(soon)(pass_on)
    phase('fwait')
    fcp.wait_recv()

    phase('qproj')
    for c in cwq:
        c.wait()
    accq[...] = mm(h_all[...], wq_s[:, 0:Q2])[0:T2]
    for c in cdw[3:]:
        c.start(priority=1)
    phase('qrope')
    cscp.wait_recv()
    even2 = lax.rem(lax.broadcasted_iota(jnp.int32, (T2, HEAD_DIM), 1), 2) == 0
    for j in range(6):
        cols = slice(j * HEAD_DIM, (j + 1) * HEAD_DIM)
        q_my[j // 3, :, (j % 3) * HEAD_DIM:(j % 3 + 1) * HEAD_DIM] = rope(
            accq[:, cols].astype(BF16).astype(F32), cs_s[0], cs_s[1], even2)
    prow = pl.ds(pl.multiple_of((x // 2) * T2, T2), T2)

    def qcopy(n):
        return rcopy(q_my.at[n], q_all.at[prow], qs.at[n], qr.at[x // 2], (tp, cp - x + 2 * par + n))

    def qlocal(n):
        q_all[prow, :] = q_my[n]

    def qarrive(i):
        rcopy(q_my.at[0], q_all.at[pl.ds(i * T2, T2)], qs.at[0], qr.at[i], pair).wait_recv()

    for n in range(2):
        when(2 * par + n != x, lambda n=n: qcopy(n).start())
        when(2 * par + n == x, lambda n=n: qlocal(n))
    def gate_up(i):
        phase(f'gu{i}')
        cols = slice(i * FC, (i + 1) * FC)
        cgu[2 * i].wait()
        g = mm(h_all[...], wg_s[:, cols])[0:T2].astype(BF16).astype(F32)
        cgu[2 * i + 1].wait()
        u = mm(h_all[...], wu_s[:, cols])[0:T2].astype(BF16).astype(F32)
        a_my[:, cols] = (g * jax.nn.sigmoid(g) * u).astype(BF16)
        acopy(i).start()
        a_cat[0:T, pl.ds(pl.multiple_of(par * FF + i * FC, FC), FC)] = a_my[mine, cols]
    phase('k1b')
    pl.when(next_)(pass_on)
    gate_up(0)
    phase('k1c')
    pl.when(third)(pass_on)
    gate_up(1)
    phase('k1d')
    pl.when(last)(pass_on)
    for c in co:
        c.start(priority=1)

    phase('qwait')
    for i in range(2):
        when(2 * i + x // 2 != x, lambda i=i: qarrive(i))
    q3 = jnp.concatenate([q_all[:, g * HEAD_DIM:(g + 1) * HEAD_DIM] for g in range(3)], axis=0)

    def scores(zz):
        kz = kv_all[0, zz].reshape(512, HEAD_DIM)
        return lax.dot_general(q3, kz, (((1,), (1,)), ((), ())), preferred_element_type=F32)

    for d in RING:
        when(v20_in[d], lambda d=d: v2(0, d).wait_recv())
    phase('row0')
    row_tok = y * R + jnp.concatenate([lax.broadcasted_iota(jnp.int32, (R, 512), 0)] * 3, axis=0)
    col_tok = lax.broadcasted_iota(jnp.int32, (3 * R, 512), 1)
    s = jnp.where(col_tok <= row_tok, scores(z), NEG)
    m0 = jnp.max(s, axis=-1, keepdims=True)
    e = jnp.exp2((s - m0) * SCALE)
    mx_s[...] = m0
    sum_s[...] = jnp.sum(e, axis=-1, keepdims=True)
    acc_s[...] = mm(e.astype(BF16), kv_all[1, z].reshape(512, HEAD_DIM))

    def mcopy(i):
        b = pl.ds(groups[i][1], NG)
        return rcopy(m_my.at[:, b], m_oth.at[:, b], ds_.at[i], dr.at[i], mate)

    def down(i):
        ref, at = groups[i]
        cdw[i].wait()
        m_my[:, at:at + NG] = (mm(a_cat[:, LO:], ref[...])[0:T] + mm(a_cat[:, 0:LO], wda_s[:, at:at + NG])[0:T]).astype(BF16)
        mcopy(i).start()

    def pcopy(i):
        b = pl.ds(i * 1024, 1024)
        return rcopy(p_my.at[:, b], p_oth.at[:, b], ds_.at[6 + i], dr.at[6 + i], mate)

    def first_down():
        for i in range(2):
            acopy(i).wait_recv()
        cda.wait()
        for i in range(2):
            down(i)

    for dz in RING:
        phase(f'row{dz}')

        @pl.when(z_in[dz])
        def _(dz=dz):
            zz = z - dz
            for dy in (0,) + RING:
                k2(dy, dz).wait_recv()
            for dy in RING:
                v2(dz, dy).wait_recv()
            s = scores(zz)
            m_old = mx_s[...]
            m_new = jnp.maximum(m_old, jnp.max(s, axis=-1, keepdims=True))
            e = jnp.exp2((s - m_new) * SCALE)
            f = jnp.exp2((m_old - m_new) * SCALE)
            mx_s[...] = m_new
            sum_s[...] = sum_s[...] * f + jnp.sum(e, axis=-1, keepdims=True)
            acc_s[...] = acc_s[...] * f + mm(e.astype(BF16), kv_all[1, zz].reshape(512, HEAD_DIM))

    phase('osend')
    o3 = (acc_s[...] / sum_s[...]).astype(BF16)
    for g in range(3):
        o_my[:, g * HEAD_DIM:(g + 1) * HEAD_DIM] = o3[g * R:(g + 1) * R]
    ocol = pl.ds(pl.multiple_of(x * GW, GW), GW)
    ocp = []
    for d in RING:
        rows = pl.ds(pl.multiple_of(lax.rem(x + d, 4) * T, T), T)
        c = rcopy(o_my.at[rows], o_cat.at[pl.ds(0, T), ocol], os_.at[d - 1], orr.at[d - 1], xp(d))
        c.start()
        ocp.append(c)
    o_cat[0:T, ocol] = o_my[myrows, :]
    out_k[...] = kx[...].astype(BF16)
    out_v[...] = vx[...].astype(BF16)

    phase('down0')
    first_down()
    down(2)
    phase('down1')
    for i in range(3, 6):
        down(i)
    phase('owait')
    for c in ocp:
        c.wait_recv()
    for i in range(3):
        phase(f'wo{i}')
        pcols = slice(i * 1024, (i + 1) * 1024)
        co[i].wait()
        p_my[:, pcols] = mm(o_cat[...], woref[i][...])[0:T].astype(BF16)
        pcopy(i).start()
    phase('final')

    order = (3, 4, 5, 1, 2, 0)

    def final(i):
        cols = slice(groups[i][1], groups[i][1] + NG)
        mcopy(i).wait_recv()
        out_h[:, cols] = (hid_s[:, cols].astype(F32) + (p_my[:, cols].astype(F32) + p_oth[:, cols].astype(F32))
                          + (m_my[:, cols].astype(F32) + m_oth[:, cols].astype(F32))).astype(BF16)

    for i in range(3):
        pcopy(i).wait_recv()
        final(order[2 * i])
        final(order[2 * i + 1])

    phase('drain')
    for n in range(2):
        when(2 * par + n != x, lambda n=n: qcopy(n).wait_send())
    for c in [hcp, fcp, cscp] + list(kcp.values()) + ocp + [mcopy(i) for i in range(6)] + [pcopy(i) for i in range(3)]:
        c.wait_send()
    for i in range(2):
        acopy(i).wait_send()
    for d in RING:
        when(k1_out[d], lambda d=d: k1(d).wait_send())
        when(v20_out[d], lambda d=d: v2(0, d).wait_send())

        for dy in range(4):
            when(z_out[d], lambda d=d, dy=dy: k2(dy, d).wait_send())
        when(z_out[d], lambda d=d: v1(d).wait_send())

        @pl.when(z_in[d])
        def _(d=d):
            for dy in RING:
                v2(d, dy).wait_send()
    phase(None)


def emit(h, k, v, out_h, out_k, out_v, sem):
    cps = [pltpu.make_async_copy(a, b, sem.at[i]) for i, (a, b) in enumerate(((h, out_h), (k, out_k), (v, out_v)))]
    for c in cps:
        c.start()
    for c in cps:
        c.wait()


def solution(mesh):
    inv = (1.0 / (np.float32(ROPE_BASE) ** (np.arange(0, HEAD_DIM, 2, dtype=np.float32) / np.float32(HEAD_DIM)))).astype(np.float32)
    inv = np.repeat(inv, 2).reshape(1, HEAD_DIM)

    def local_layer(hidden, positions, ln_gain, w_q, w_k, w_v, w_o, w_gate, w_up, w_down):
        vm = pl.BlockSpec(memory_space=pltpu.VMEM)
        hb = pl.BlockSpec(memory_space=pl.ANY)
        dma = pltpu.SemaphoreType.DMA
        V = pltpu.VMEM
        scratch = [
            V((T, D), BF16), V((1, T), jnp.int32), V((D // HEAD_DIM, HEAD_DIM), BF16), V((1, HEAD_DIM), F32),
            V((D, QW), BF16), V((D, KW), BF16), V((D, KW), BF16),
            V((D, FF), BF16), V((D, FF), BF16), V((LO, D), BF16), V((D, KW), BF16),
            V((R, D), BF16), V((2, T2, HEAD_DIM), F32), V((T2, Q2), F32), V((T, KW), F32), V((T, KW), F32), V((R, HEAD_DIM), F32), V((R, HEAD_DIM), F32),
            V((2, T2, GW), BF16), V((R, GW), BF16), V((4, 2, T, HEAD_DIM), BF16), V((2, 4, 4, R, HEAD_DIM), BF16),
            V((3 * R, 1), F32), V((3 * R, 1), F32), V((3 * R, HEAD_DIM), F32), V((R, GW), BF16), V((R, QW), BF16),
            V((T2, FF), BF16), V((R, FFT), BF16), V((T, D), BF16), V((T, D), BF16), V((T, D), BF16), V((T, D), BF16),
            dma((4,)), dma((26,)), dma((2,)), dma((3,)), dma((3,)), dma((3,)), dma((3,)), dma((3,)), dma((3,)), dma((3,)), dma((3,)),
            dma((3,)), dma((3,)), dma((3,)), dma((3,)), dma((12,)), dma((12,)), dma((12,)), dma((12,)),
            dma((6,)), dma((6,)), dma((3,)), dma((3,)), dma((9,)), dma((9,)),
        ]
        outs = (jax.ShapeDtypeStruct((T, D), BF16), jax.ShapeDtypeStruct((R, HEAD_DIM), BF16), jax.ShapeDtypeStruct((R, HEAD_DIM), BF16))
        res = pl.pallas_call(
            kernel,
            name='layer',
            out_shape=tuple(pltpu.VMEM(o.shape, o.dtype) for o in outs),
            in_specs=[hb] * 11,
            out_specs=(vm, vm, vm),
            scratch_shapes=scratch,
            compiler_params=pltpu.CompilerParams(collective_id=0, has_side_effects=True, vmem_limit_bytes=60000000),
        )(hidden, positions.reshape(1, T), ln_gain.reshape(D // HEAD_DIM, HEAD_DIM), jnp.asarray(inv),
          w_q, w_k, w_v, w_o, w_gate, w_up, w_down)
        out_h, out_k, out_v = pl.pallas_call(
            emit,
            name='emit',
            out_shape=outs,
            in_specs=[vm] * 3,
            out_specs=(hb, hb, hb),
            scratch_shapes=[dma((3,))],
        )(*[pltpu.with_memory_space_constraint(r, pltpu.VMEM) for r in res])
        return out_h, out_k.reshape(T, 4, HEAD_DIM), out_v.reshape(T, 4, HEAD_DIM)

    row_spec = P(('dp', 'cp'), None)
    col_spec = P(None, 'tp')
    cache_spec = P(('dp', 'cp'), 'tp', None)
    in_specs = (row_spec, P(('dp', 'cp')), P(None), col_spec, col_spec, col_spec, P('tp', None), col_spec, col_spec, P('tp', None))
    return jax.shard_map(local_layer, mesh=mesh, in_specs=in_specs, out_specs=(row_spec, cache_spec, cache_spec), check_vma=False)
```

```python
import jax
import jax.numpy as jnp
import numpy as np
from jax import lax
from jax.experimental import pallas as pl
from jax.experimental.pallas import tpu as pltpu
from jax.sharding import PartitionSpec as P

HEAD_DIM = 128
ROPE_BASE = 4000000
LN_EPS = 1e-5
D = 3072
T = 32
R = 128
QW = 1536
KW = 512
GW = 384
T2 = 64
FF = 2048
FC = 1024
LO = 1024
FFT = 4096
KC = 2
Q2 = 768
NG = 512
NEG = -1e30
SCALE = HEAD_DIM ** -0.5 * 1.4426950408889634
F32 = jnp.float32
BF16 = jnp.bfloat16
RING = (1, 3, 2)


def mm(a, b):
    return jnp.dot(a, b, preferred_element_type=F32)


def rope(x, cos, sin, even):
    left = pltpu.roll(x, 127, 1)
    right = pltpu.roll(x, 1, 1)
    return (x * cos + jnp.where(even, -left, right) * sin).astype(BF16)


def kernel(hid, pos, gain, invf, wq, wk, wv, wo, wg, wu, wd,
           out_h, out_k, out_v,
           hid_s, pos_s, gain_s, inv_s,
           wq_s, wk_s, wv_s, wg_s, wu_s, wda_s, wdx_s,
           h_all, cs_s, accq, acck, accv, kx, vx, q_my, q_all, kv_my, kv_all,
           mx_s, sum_s, acc_s, o_my, o_cat,
           a_my, a_cat, m_my, m_oth, p_my, p_oth,
           i_sem, w_sem, cs_sem, hs, hr, fs, fr, qs, qr, ks, kr, k1s, k1r, v1s, v1r, k2s, k2r, v2s, v2r,
           as_, ar, os_, orr, ds_, dr):
    scope = []

    def phase(name):
        if scope:
            scope.pop().__exit__(None, None, None)
        if name:
            scope.append(jax.named_scope(name))
            scope[0].__enter__()

    phase('start')
    tp = lax.axis_index('tp')
    cp = lax.axis_index('cp')
    x = lax.rem(cp, 4)
    y = lax.rem(cp // 4, 4)
    z = cp // 16

    def xp(d):
        return tp, z * 16 + y * 4 + lax.rem(x + d, 4)

    def yp(d):
        return tp, z * 16 + lax.rem(y + d, 4) * 4 + x

    def zp(d):
        return tp, lax.rem(z + d, 4) * 16 + y * 4 + x

    mate = (1 - tp, cp)

    def when(cond, fn):
        pl.when(cond)(lambda: fn())

    def rcopy(src, dst, ss, rs, dev):
        return pltpu.make_async_remote_copy(
            src_ref=src, dst_ref=dst, send_sem=ss, recv_sem=rs,
            device_id={'tp': dev[0], 'cp': dev[1]}, device_id_type=pl.DeviceIdType.MESH)

    small = [pltpu.make_async_copy(a, b, i_sem.at[i])
             for i, (a, b) in enumerate(((hid, hid_s), (gain, gain_s), (pos, pos_s), (invf, inv_s)))]
    for c in small:
        c.start()
    half = D // 2
    ckv = [pltpu.make_async_copy(src.at[pl.ds(i * half, half)], dst.at[pl.ds(i * half, half)], w_sem.at[2 * i + n])
           for i in range(2) for n, (src, dst) in enumerate(((wk, wk_s), (wv, wv_s)))]
    kc = D // KC
    par = lax.rem(x, 2)
    pair = (tp, cp + 1 - 2 * par)
    qcol = pl.ds(pl.multiple_of(par * Q2, Q2), Q2)
    cwq = [pltpu.make_async_copy(wq.at[pl.ds(i * kc, kc), qcol], wq_s.at[pl.ds(i * kc, kc), pl.ds(0, Q2)], w_sem.at[4 + i]) for i in range(KC)]
    mine = pl.ds(pl.multiple_of(par * T, T), T)
    theirs = pl.ds(pl.multiple_of((1 - par) * T, T), T)
    hcol = pl.ds(pl.multiple_of(tp * QW, QW), QW)
    cgu = [pltpu.make_async_copy(src.at[:, pl.ds(pl.multiple_of(par * FF + i * FC, FC), FC)],
                                 dst.at[:, pl.ds(i * FC, FC)], w_sem.at[8 + 2 * i + n])
           for i in range(2) for n, (src, dst) in enumerate(((wg, wg_s), (wu, wu_s)))]
    cda = pltpu.make_async_copy(wd.at[pl.ds(0, LO)], wda_s, w_sem.at[16])
    woref = [wg_s.at[pl.ds(0, QW), pl.ds(0, 1024)], wg_s.at[pl.ds(0, QW), pl.ds(1024, 1024)], wg_s.at[pl.ds(QW, QW), pl.ds(0, 1024)]]
    co = [pltpu.make_async_copy(wo.at[:, pl.ds(i * 1024, 1024)], woref[i], w_sem.at[17 + i]) for i in range(3)]
    pieces = [(wdx_s.at[:], 5 * NG), (wk_s.at[:], 3 * NG), (wv_s.at[:], 4 * NG)] + [
        (wq_s.at[:, pl.ds(i * NG, NG)], i * NG) for i in range(3)]
    groups = [(wdx_s, 5 * NG, NG), (wk_s, 3 * NG, NG), (wv_s, 4 * NG, NG), (wq_s, 0, 3 * NG)]
    low = pl.ds(LO, D)
    cdw = [pltpu.make_async_copy(wd.at[low, pl.ds(at, NG)], ref, w_sem.at[20 + i]) for i, (ref, at) in enumerate(pieces)]
    for c in ckv:
        c.start(priority=1)

    barrier = pltpu.get_barrier_semaphore()
    peers = [f(d) for f in (xp, yp, zp) for d in (1, 2, 3)] + [mate]
    for dev in peers:
        pl.semaphore_signal(barrier, inc=1, device_id={'tp': dev[0], 'cp': dev[1]}, device_id_type=pl.DeviceIdType.MESH)

    h_all[T2:R, :] = jnp.zeros((R - T2, D), BF16)
    a_cat[T:R, :] = jnp.zeros((R - T, FFT), BF16)
    o_cat[T:R, :] = jnp.zeros((R - T, QW), BF16)

    for yy in range(4):
        @pl.when(yy > y)
        def _(yy=yy):
            kv_all[1, z, yy] = jnp.zeros((R, HEAD_DIM), BF16)

        @pl.when(jnp.logical_and(yy > y, z == 3))
        def _(yy=yy):
            kv_all[0, z, yy] = jnp.zeros((R, HEAD_DIM), BF16)

    phase('ln')
    for c in small:
        c.wait()
    for c in cwq + cgu + [cda, cdw[0]]:
        c.start(priority=1)
    hf = hid_s[...].astype(F32)
    mean = jnp.sum(hf, axis=-1, keepdims=True) * (1.0 / D)
    cen = hf - mean
    var = jnp.sum(cen * cen, axis=-1, keepdims=True) * (1.0 / D)
    scaled = cen * lax.rsqrt(var + LN_EPS)
    gf = gain_s[...].astype(F32)
    myrows = pl.ds(pl.multiple_of(x * T, T), T)
    for i in range(D // HEAD_DIM):
        cols = slice(i * HEAD_DIM, (i + 1) * HEAD_DIM)
        h_all[mine, cols] = (scaled[:, cols] * gf[i:i + 1]).astype(BF16)

    hcp = rcopy(h_all.at[mine, hcol], h_all.at[mine, hcol], hs.at[0], hr.at[0], pair)
    fcp = rcopy(h_all.at[theirs, hcol], h_all.at[theirs, hcol], fs.at[0], fr.at[0], mate)
    kcp = {d: rcopy(kv_my.at[lax.rem(x + d, 4)], kv_all.at[:, z, y, myrows], ks.at[d - 1], kr.at[d - 1], xp(d)) for d in RING}

    phase('tables')
    diag = lax.broadcasted_iota(jnp.int32, (T, T), 0) == lax.broadcasted_iota(jnp.int32, (T, T), 1)
    posf = jnp.sum(jnp.where(diag, jnp.broadcast_to(pos_s[...].astype(F32), (T, T)), 0.0), axis=1, keepdims=True)
    ang = posf * inv_s[...]
    cos = jnp.cos(ang)
    sin = jnp.sin(ang)
    even = lax.rem(lax.broadcasted_iota(jnp.int32, (T, HEAD_DIM), 1), 2) == 0
    cs_s[0, mine] = cos
    cs_s[1, mine] = sin
    cscp = rcopy(cs_s.at[:, mine], cs_s.at[:, mine], cs_sem.at[0], cs_sem.at[1], pair)

    phase('kvproj')
    for i in range(2):
        rows = slice(i * half, (i + 1) * half)
        for n, (w, acc) in enumerate(((wk_s, acck), (wv_s, accv))):
            ckv[2 * i + n].wait()
            part = mm(h_all[mine, rows], w[rows, :])
            if i == 0:
                acc[...] = part
            else:
                acc[...] += part
    phase('kvrope')
    for j in range(4):
        cols = slice(j * HEAD_DIM, (j + 1) * HEAD_DIM)
        kj = rope(acck[:, cols].astype(BF16).astype(F32), cos, sin, even)
        vj = accv[:, cols].astype(BF16)
        kv_my[j, 0] = kj
        kv_my[j, 1] = vj
        kx[pl.ds(j, T, stride=4), :] = kj.astype(F32)
        vx[pl.ds(j, T, stride=4), :] = vj.astype(F32)
    kv_all[:, z, y, myrows, :] = kv_my[x]

    phase('barrier')
    pl.semaphore_wait(barrier, len(peers))
    for d in RING:
        kcp[d].start()
    hcp.start()
    cscp.start()

    for c in cdw[1:3]:
        c.start(priority=1)

    def k1(d):
        b = kv_all.at[0, z, y]
        return rcopy(b, b, k1s.at[d - 1], k1r.at[d - 1], yp(d))

    def v1(d):
        b = kv_all.at[1, z, y]
        return rcopy(b, b, v1s.at[d - 1], v1r.at[d - 1], zp(d))

    def k2(dy, dz):
        b = kv_all.at[0, z, lax.rem(y + 4 - dy, 4)]
        return rcopy(b, b, k2s.at[3 * dy + dz - 1], k2r.at[3 * dy + dz - 1], zp(dz))

    def v2(dz, dy):
        b = kv_all.at[1, lax.rem(z + 4 - dz, 4), y]
        return rcopy(b, b, v2s.at[3 * dz + dy - 1], v2r.at[3 * dz + dy - 1], yp(dy))

    k1_out = {d: jnp.logical_or(y + d <= 3, z < 3) for d in RING}
    k1_in = {d: jnp.logical_or(y >= d, z < 3) for d in RING}
    z_out = {d: z + d <= 3 for d in RING}
    z_in = {d: z >= d for d in RING}
    v20_out = {d: y + d <= 3 for d in RING}
    v20_in = {d: y >= d for d in RING}

    phase('kvx')
    for d in RING:
        kcp[d].wait_recv()
    for d in RING:
        when(k1_out[d], lambda d=d: k1(d).start())
        when(z_out[d], lambda d=d: v1(d).start())
    for d in RING:
        when(z_out[d], lambda d=d: k2(0, d).start())
    for d in RING:
        when(v20_out[d], lambda d=d: v2(0, d).start())

    phase('hwait')
    hcp.wait_recv()
    fcp.start()

    def acopy(i):
        cols = pl.ds(pl.multiple_of(par * FF + i * FC, FC), FC)
        return rcopy(a_my.at[theirs, pl.ds(i * FC, FC)], a_cat.at[pl.ds(0, T), cols], as_.at[i], ar.at[i], pair)

    def pass_on():
        for d in RING:
            when(k1_in[d], lambda d=d: k1(d).wait_recv())
            for dz in RING:
                when(z_out[dz], lambda d=d, dz=dz: k2(d, dz).start())

            @pl.when(z_in[d])
            def _(d=d):
                v1(d).wait_recv()
                for dy in RING:
                    v2(d, dy).start()

    soon = jnp.logical_and(tp == 1, y >= 1)
    next_ = jnp.logical_and(tp == 0, y >= 2)
    last = jnp.logical_and(tp == 0, jnp.logical_and(y == 0, z == 0))
    third = jnp.logical_not(jnp.logical_or(last, jnp.logical_or(soon, next_)))

    phase('k1a')
    pl.when(soon)(pass_on)
    phase('fwait')
    fcp.wait_recv()

    phase('qproj')
    for c in cwq:
        c.wait()
    accq[...] = mm(h_all[...], wq_s[:, 0:Q2])[0:T2]
    for c in cdw[3:]:
        c.start(priority=1)
    phase('qrope')
    cscp.wait_recv()
    even2 = lax.rem(lax.broadcasted_iota(jnp.int32, (T2, HEAD_DIM), 1), 2) == 0
    for j in range(6):
        cols = slice(j * HEAD_DIM, (j + 1) * HEAD_DIM)
        q_my[j // 3, :, (j % 3) * HEAD_DIM:(j % 3 + 1) * HEAD_DIM] = rope(
            accq[:, cols].astype(BF16).astype(F32), cs_s[0], cs_s[1], even2)
    prow = pl.ds(pl.multiple_of((x // 2) * T2, T2), T2)

    def qcopy(n):
        return rcopy(q_my.at[n], q_all.at[prow], qs.at[n], qr.at[x // 2], (tp, cp - x + 2 * par + n))

    def qlocal(n):
        q_all[prow, :] = q_my[n]

    def qarrive(i):
        rcopy(q_my.at[0], q_all.at[pl.ds(i * T2, T2)], qs.at[0], qr.at[i], pair).wait_recv()

    for n in range(2):
        when(2 * par + n != x, lambda n=n: qcopy(n).start())
        when(2 * par + n == x, lambda n=n: qlocal(n))
    def gate_up(i):
        phase(f'gu{i}')
        cols = slice(i * FC, (i + 1) * FC)
        cgu[2 * i].wait()
        g = mm(h_all[...], wg_s[:, cols])[0:T2].astype(BF16).astype(F32)
        cgu[2 * i + 1].wait()
        u = mm(h_all[...], wu_s[:, cols])[0:T2].astype(BF16).astype(F32)
        a_my[:, cols] = (g * jax.nn.sigmoid(g) * u).astype(BF16)
        acopy(i).start()
        a_cat[0:T, pl.ds(pl.multiple_of(par * FF + i * FC, FC), FC)] = a_my[mine, cols]
    phase('k1b')
    pl.when(next_)(pass_on)
    gate_up(0)
    phase('k1c')
    pl.when(third)(pass_on)
    gate_up(1)
    phase('k1d')
    pl.when(last)(pass_on)
    for c in co:
        c.start(priority=1)

    phase('qwait')
    for i in range(2):
        when(2 * i + x // 2 != x, lambda i=i: qarrive(i))
    q3 = jnp.concatenate([q_all[:, g * HEAD_DIM:(g + 1) * HEAD_DIM] for g in range(3)], axis=0)

    def scores(zz):
        kz = kv_all[0, zz].reshape(512, HEAD_DIM)
        return lax.dot_general(q3, kz, (((1,), (1,)), ((), ())), preferred_element_type=F32)

    for d in RING:
        when(v20_in[d], lambda d=d: v2(0, d).wait_recv())
    phase('row0')
    row_tok = y * R + jnp.concatenate([lax.broadcasted_iota(jnp.int32, (R, 512), 0)] * 3, axis=0)
    col_tok = lax.broadcasted_iota(jnp.int32, (3 * R, 512), 1)
    s = jnp.where(col_tok <= row_tok, scores(z), NEG)
    m0 = jnp.max(s, axis=-1, keepdims=True)
    e = jnp.exp2((s - m0) * SCALE)
    mx_s[...] = m0
    sum_s[...] = jnp.sum(e, axis=-1, keepdims=True)
    acc_s[...] = mm(e.astype(BF16), kv_all[1, z].reshape(512, HEAD_DIM))

    def mcopy(i):
        b = pl.ds(groups[i][1], groups[i][2])
        return rcopy(m_my.at[:, b], m_oth.at[:, b], ds_.at[i], dr.at[i], mate)

    def down(i):
        ref, at, n = groups[i]
        for c in cdw[i:i + n // NG]:
            c.wait()
        m_my[:, at:at + n] = (mm(a_cat[:, LO:], ref[...])[0:T] + mm(a_cat[:, 0:LO], wda_s[:, at:at + n])[0:T]).astype(BF16)
        mcopy(i).start()

    def pcopy(i):
        b = pl.ds(2048 * i, 2048 - 1024 * i)
        return rcopy(p_my.at[:, b], p_oth.at[:, b], ds_.at[6 + i], dr.at[6 + i], mate)

    def first_down():
        for i in range(2):
            acopy(i).wait_recv()
        cda.wait()
        for i in range(2):
            down(i)

    for dz in RING:
        phase(f'row{dz}')

        @pl.when(z_in[dz])
        def _(dz=dz):
            zz = z - dz
            for dy in (0,) + RING:
                k2(dy, dz).wait_recv()
            for dy in RING:
                v2(dz, dy).wait_recv()
            s = scores(zz)
            m_old = mx_s[...]
            m_new = jnp.maximum(m_old, jnp.max(s, axis=-1, keepdims=True))
            e = jnp.exp2((s - m_new) * SCALE)
            f = jnp.exp2((m_old - m_new) * SCALE)
            mx_s[...] = m_new
            sum_s[...] = sum_s[...] * f + jnp.sum(e, axis=-1, keepdims=True)
            acc_s[...] = acc_s[...] * f + mm(e.astype(BF16), kv_all[1, zz].reshape(512, HEAD_DIM))

    phase('osend')
    o3 = (acc_s[...] / sum_s[...]).astype(BF16)
    for g in range(3):
        o_my[:, g * HEAD_DIM:(g + 1) * HEAD_DIM] = o3[g * R:(g + 1) * R]
    ocol = pl.ds(pl.multiple_of(x * GW, GW), GW)
    ocp = []
    for d in RING:
        rows = pl.ds(pl.multiple_of(lax.rem(x + d, 4) * T, T), T)
        c = rcopy(o_my.at[rows], o_cat.at[pl.ds(0, T), ocol], os_.at[d - 1], orr.at[d - 1], xp(d))
        c.start()
        ocp.append(c)
    o_cat[0:T, ocol] = o_my[myrows, :]
    out_k[...] = kx[...].astype(BF16)
    out_v[...] = vx[...].astype(BF16)

    phase('down0')
    first_down()
    down(2)
    phase('down1')
    down(3)
    phase('owait')
    for c in ocp:
        c.wait_recv()
    co[0].wait()
    co[1].wait()
    phase('wo0')
    p_my[:, 0:2048] = mm(o_cat[...], wg_s[0:QW, :])[0:T].astype(BF16)
    pcopy(0).start()
    co[2].wait()
    phase('wo1')
    p_my[:, 2048:D] = mm(o_cat[...], wg_s[QW:D, 0:1024])[0:T].astype(BF16)
    pcopy(1).start()
    phase('final')

    def final(cols):
        out_h[:, cols] = (hid_s[:, cols].astype(F32) + (p_my[:, cols].astype(F32) + p_oth[:, cols].astype(F32))
                          + (m_my[:, cols].astype(F32) + m_oth[:, cols].astype(F32))).astype(BF16)

    for i in range(4):
        mcopy(i).wait_recv()
    pcopy(0).wait_recv()
    final(slice(0, 2048))
    pcopy(1).wait_recv()
    final(slice(2048, D))

    phase('drain')
    for n in range(2):
        when(2 * par + n != x, lambda n=n: qcopy(n).wait_send())
    for c in [hcp, fcp, cscp] + list(kcp.values()) + ocp + [mcopy(i) for i in range(4)] + [pcopy(i) for i in range(2)]:
        c.wait_send()
    for i in range(2):
        acopy(i).wait_send()
    for d in RING:
        when(k1_out[d], lambda d=d: k1(d).wait_send())
        when(v20_out[d], lambda d=d: v2(0, d).wait_send())

        for dy in range(4):
            when(z_out[d], lambda d=d, dy=dy: k2(dy, d).wait_send())
        when(z_out[d], lambda d=d: v1(d).wait_send())

        @pl.when(z_in[d])
        def _(d=d):
            for dy in RING:
                v2(d, dy).wait_send()
    phase(None)


def emit(h, k, v, out_h, out_k, out_v, sem):
    cps = [pltpu.make_async_copy(a, b, sem.at[i]) for i, (a, b) in enumerate(((h, out_h), (k, out_k), (v, out_v)))]
    for c in cps:
        c.start()
    for c in cps:
        c.wait()


def solution(mesh):
    inv = (1.0 / (np.float32(ROPE_BASE) ** (np.arange(0, HEAD_DIM, 2, dtype=np.float32) / np.float32(HEAD_DIM)))).astype(np.float32)
    inv = np.repeat(inv, 2).reshape(1, HEAD_DIM)

    def local_layer(hidden, positions, ln_gain, w_q, w_k, w_v, w_o, w_gate, w_up, w_down):
        vm = pl.BlockSpec(memory_space=pltpu.VMEM)
        hb = pl.BlockSpec(memory_space=pl.ANY)
        dma = pltpu.SemaphoreType.DMA
        V = pltpu.VMEM
        scratch = [
            V((T, D), BF16), V((1, T), jnp.int32), V((D // HEAD_DIM, HEAD_DIM), BF16), V((1, HEAD_DIM), F32),
            V((D, QW), BF16), V((D, KW), BF16), V((D, KW), BF16),
            V((D, FF), BF16), V((D, FF), BF16), V((LO, D), BF16), V((D, KW), BF16),
            V((R, D), BF16), V((2, T2, HEAD_DIM), F32), V((T2, Q2), F32), V((T, KW), F32), V((T, KW), F32), V((R, HEAD_DIM), F32), V((R, HEAD_DIM), F32),
            V((2, T2, GW), BF16), V((R, GW), BF16), V((4, 2, T, HEAD_DIM), BF16), V((2, 4, 4, R, HEAD_DIM), BF16),
            V((3 * R, 1), F32), V((3 * R, 1), F32), V((3 * R, HEAD_DIM), F32), V((R, GW), BF16), V((R, QW), BF16),
            V((T2, FF), BF16), V((R, FFT), BF16), V((T, D), BF16), V((T, D), BF16), V((T, D), BF16), V((T, D), BF16),
            dma((4,)), dma((26,)), dma((2,)), dma((3,)), dma((3,)), dma((3,)), dma((3,)), dma((3,)), dma((3,)), dma((3,)), dma((3,)),
            dma((3,)), dma((3,)), dma((3,)), dma((3,)), dma((12,)), dma((12,)), dma((12,)), dma((12,)),
            dma((6,)), dma((6,)), dma((3,)), dma((3,)), dma((9,)), dma((9,)),
        ]
        outs = (jax.ShapeDtypeStruct((T, D), BF16), jax.ShapeDtypeStruct((R, HEAD_DIM), BF16), jax.ShapeDtypeStruct((R, HEAD_DIM), BF16))
        res = pl.pallas_call(
            kernel,
            name='layer',
            out_shape=tuple(pltpu.VMEM(o.shape, o.dtype) for o in outs),
            in_specs=[hb] * 11,
            out_specs=(vm, vm, vm),
            scratch_shapes=scratch,
            compiler_params=pltpu.CompilerParams(collective_id=0, has_side_effects=True, vmem_limit_bytes=60000000),
        )(hidden, positions.reshape(1, T), ln_gain.reshape(D // HEAD_DIM, HEAD_DIM), jnp.asarray(inv),
          w_q, w_k, w_v, w_o, w_gate, w_up, w_down)
        out_h, out_k, out_v = pl.pallas_call(
            emit,
            name='emit',
            out_shape=outs,
            in_specs=[vm] * 3,
            out_specs=(hb, hb, hb),
            scratch_shapes=[dma((3,))],
        )(*[pltpu.with_memory_space_constraint(r, pltpu.VMEM) for r in res])
        return out_h, out_k.reshape(T, 4, HEAD_DIM), out_v.reshape(T, 4, HEAD_DIM)

    row_spec = P(('dp', 'cp'), None)
    col_spec = P(None, 'tp')
    cache_spec = P(('dp', 'cp'), 'tp', None)
    in_specs = (row_spec, P(('dp', 'cp')), P(None), col_spec, col_spec, col_spec, P('tp', None), col_spec, col_spec, P('tp', None))
    return jax.shard_map(local_layer, mesh=mesh, in_specs=in_specs, out_specs=(row_spec, cache_spec, cache_spec), check_vma=False)
```
